32 devices in a mesh: row: 4 (over y, x), col: 8 (over z, core).
Axes of the slice: x: 2, y: 2, z: 4, core: 2. Of those that a mesh axis runs over, the one named last changes fastest.
Arguments:
- layer_input: bfloat16 [8192, 2048], P(('row', 'col')), may hold values from -6 to 6
- out_grad: bfloat16 [8192, 2048], P(('row', 'col')), may hold values from -6 to 6
- kv_grad: bfloat16 [8192, 256], P(('row', 'col')), may hold values from -6 to 6
- lengths: int32 [4, 4], P('row'), may hold values from 1 to 1024, 2048 in all within a row
- token_deal: int32 [4, 2048], P('row'), may hold values from 0 to 2047, each once within a row
- attn_gain: float32 [2048], P('row'), may hold values from 0.25 to 1.75
- query_weight: float32 [2048, 2048], P('row', 'col'), may hold values from -0.125 to 0.125
- key_weight: float32 [2048, 128], P('row'), may hold values from -0.125 to 0.125
- value_weight: float32 [2048, 128], P('row'), may hold values from -0.125 to 0.125
- out_weight: float32 [2048, 2048], P('col', 'row'), may hold values from -1 to 1
- mlp_gain: float32 [2048], P('row'), may hold values from 0.25 to 1.75
- gate_weight: float32 [2048, 5632], P('row', 'col'), may hold values from -0.125 to 0.125
- up_weight: float32 [2048, 5632], P('row', 'col'), may hold values from -0.125 to 0.125
- down_weight: float32 [5632, 2048], P('col', 'row'), may hold values from -0.3125 to 0.3125
Outputs:
- layer_output: bfloat16 [8192, 2048], P(('row', 'col'))
- input_grad: float32 [8192, 2048], P(('row', 'col'))
- shared_kv: bfloat16 [8192, 256], P(('row', 'col'))
- attn_gain_grad: float32 [2048], P('row')
- query_weight_grad: float32 [2048, 2048], P('row', 'col')
- key_weight_grad: float32 [2048, 128], P('row')
- value_weight_grad: float32 [2048, 128], P('row')
- out_weight_grad: float32 [2048, 2048], P('col', 'row')
- mlp_gain_grad: float32 [2048], P('row')
- gate_weight_grad: float32 [2048, 5632], P('row', 'col')
- up_weight_grad: float32 [2048, 5632], P('row', 'col')
- down_weight_grad: float32 [5632, 2048], P('col', 'row')
The draws below stay inside these ranges and needn't reach their ends.
Inputs may be any that keep to these rules, and one draw needn't show every extreme that they name: Each row holds 4 lengths that sum to 2048; the longest of each row is exactly 1024. `token_deal`: each row is a permutation of 0 to 2047.
All inputs are finite; a program needn't handle non-finite values.
Results may differ from the reference program's by a relative error of at most 0.017.
The reference program's roundings to bfloat16 on the way count: a program that leaves them out, or rounds other values in their place, can miss the bound.
Values may be sent and summed in bfloat16 or wider, within the bound.
No kernel may reach another device: no remote copies, remote signals or barrier semaphores. Data moves between devices by JAX's collectives and lax.ppermute only.
A program may use at most 320 MiB of HBM per device.

```python
import math
import jax
import jax.numpy as jnp
import numpy as np
from jax import lax

D = 2048
HEADS = 16
HD = 128
FF = 5632
SEQS = 4
GROUP = 2048
GROUPS = 4
TOKENS = 8192
MOST = 1024


def level_of(key, shape, cuts, least, top_value):
    level, own = 1.0, jax.random.fold_in(key, 6)
    for axis_at, shards_of in cuts:
        steps = jnp.exp(jax.random.uniform(jax.random.fold_in(own, axis_at), (shards_of,), jnp.float32, least / len(cuts), top_value / len(cuts)))
        level = level * jnp.repeat(steps, shape[axis_at] // shards_of).reshape([-1 if axis == axis_at else 1 for axis in range(len(shape))])
    return level


def split_up(count, total, bound, lean):
    loads = [(1 << 20) // math.isqrt(grade ** lean) + 1 for grade in range(2, count + 1)]
    spare, holding = total - bound - (count - 1), [1] * (count - 1)
    while spare > 0:
        candidates = [i for i in range(count - 1) if holding[i] < bound]
        whole, left = sum([loads[i] for i in candidates]), spare
        for i in candidates:
            extra = min(bound - holding[i], max(1, left * loads[i] // whole), spare)
            holding[i] = holding[i] + extra
            spare = spare - extra
    return np.array([bound] + holding)


def ragged_sizes(rng, number_of, total, most, lean):
    if number_of == 2:
        one = jax.random.randint(rng, (), max(1, total - most), min(most, total - 1) + 1)
        return jnp.stack([one, total - one])
    sizes = jnp.asarray(split_up(number_of, total, most, lean), jnp.int32)
    couples = (number_of - 1) // 2
    giver, taker = sizes[1:1 + 2 * couples:2], sizes[2:2 + 2 * couples:2]
    margin = jnp.minimum(giver - 1, most - taker)
    moved = jax.random.randint(jax.random.fold_in(rng, 1), (couples,), 0, 1 << 20) % (margin + 1)
    sizes = sizes.at[1:1 + 2 * couples:2].set(giver - moved).at[2:2 + 2 * couples:2].set(taker + moved)
    return sizes[jax.random.permutation(jax.random.fold_in(rng, 2), number_of)]


def normal_values(key, shape, width, limit, shards=(), held_as=jnp.bfloat16):
    array = jax.random.normal(key, shape, jnp.float32) * width
    if len(shards) > 0:
        array = level_of(key, shape, shards, -0.22, 0.18) * array
    return jnp.clip(array, min=-limit, max=limit).astype(held_as)


def setup_inputs(seed: int = 0) -> dict:
    key_of = jax.random.split(jax.random.key(seed), 15)
    return {
        "layer_input": normal_values(key_of[0], (TOKENS, D), 1.0, 6.0, ((0, 32),)),
        "out_grad": normal_values(key_of[1], (TOKENS, D), 1.0, 6.0, ((0, 32),)),
        "kv_grad": normal_values(key_of[2], (TOKENS, 2 * HD), 1.0, 6.0, ((0, 32),)),
        "lengths": jax.vmap(lambda own: ragged_sizes(own, SEQS, GROUP, MOST, 2))(jax.random.split(key_of[3], GROUPS)).reshape((GROUPS, SEQS)).astype(jnp.int32),
        "token_deal": jax.vmap(lambda own: jax.random.permutation(own, GROUP))(jax.random.split(key_of[4], GROUPS)).reshape((GROUPS, GROUP)).astype(jnp.int32),
        "attn_gain": jnp.clip(1.0 + 0.15 * jax.random.normal(key_of[5], (D,), jnp.float32), 0.25, 1.75),
        "query_weight": normal_values(key_of[6], (D, HEADS * HD), D ** -0.5, 0.125, ((0, 4), (1, 8)), jnp.float32),
        "key_weight": normal_values(key_of[7], (D, HD), D ** -0.5, 0.125, ((0, 4),), jnp.float32),
        "value_weight": normal_values(key_of[8], (D, HD), D ** -0.5, 0.125, ((0, 4),), jnp.float32),
        "out_weight": normal_values(key_of[9], (HEADS * HD, D), (HEADS * HD // 64) ** -0.5, 1.0, ((0, 8), (1, 4)), jnp.float32),
        "mlp_gain": jnp.clip(1.0 + 0.15 * jax.random.normal(key_of[10], (D,), jnp.float32), 0.25, 1.75),
        "gate_weight": normal_values(key_of[11], (D, FF), D ** -0.5, 0.125, ((0, 4), (1, 8)), jnp.float32),
        "up_weight": normal_values(key_of[12], (D, FF), D ** -0.5, 0.125, ((0, 4), (1, 8)), jnp.float32),
        "down_weight": normal_values(key_of[13], (FF, D), (FF // 16) ** -0.5, 0.3125, ((0, 8), (1, 4)), jnp.float32),
    }


norm_eps = 1e-05
rope_base = 10000.0
masked_score = -1e+30

@jax.custom_vjp
def low(v):
    return lax.optimization_barrier(v.astype(jnp.bfloat16)).astype(jnp.float32)

@jax.custom_vjp
def low_back(v):
    return v

def low_keep(v):
    return (low(v), None)

def low_pass(kept, grad):
    return (grad,)

def back_keep(v):
    return (v, None)

def back_low(kept, grad):
    return (low(grad),)
low.defvjp(low_keep, low_pass)
low_back.defvjp(back_keep, back_low)

def matmul(left, right):
    return jnp.dot(left, right, precision=lax.Precision.HIGHEST, preferred_element_type=jnp.float32)

def rms_normed(values, gain):
    factor = lax.rsqrt(lax.optimization_barrier(jnp.mean(values * values, axis=-1, keepdims=True)) + norm_eps)
    return values * factor * gain

def rotate_pairs(values, positions):
    half_dim = values.shape[-1] // 2
    frequency = rope_base ** (-jnp.arange(half_dim, dtype=jnp.float32) / half_dim)
    angles = positions.astype(jnp.float32)[:, None, None] * frequency
    cosine = jnp.cos(angles)
    sine_part = jnp.sin(angles)
    first_half = values[..., :half_dim]
    second = values[..., half_dim:]
    return jnp.concatenate([first_half * cosine - second * sine_part, second * cosine + first_half * sine_part], axis=-1)

def attend_group(queries, key_rows, value_rows, seq_ids):
    block_rows = min(512, GROUP)
    score_scale = HD ** (-0.5)
    key_index = jnp.arange(GROUP, dtype=jnp.int32)

    def one_block(block_index):
        first_row = block_index * block_rows
        query_block = lax.dynamic_slice_in_dim(queries, first_row, block_rows, 0)
        row_index = first_row + jnp.arange(block_rows, dtype=jnp.int32)
        row_seq = lax.dynamic_slice_in_dim(seq_ids, first_row, block_rows, 0)
        scores = jnp.einsum('qhd,kd->hqk', query_block, key_rows, precision=lax.Precision.HIGHEST) * score_scale
        scores = low_back(scores)
        allowed = (row_seq[:, None] == seq_ids[None, :]) & (key_index[None, :] <= row_index[:, None])
        scores = jnp.where(allowed[None], scores, masked_score)
        weights = low(jax.nn.softmax(scores, axis=-1))
        mixed_rows = jnp.einsum('hqk,kd->qhd', weights, value_rows, precision=lax.Precision.HIGHEST)
        return low(low_back(mixed_rows))
    blocks = lax.map(jax.checkpoint(one_block), jnp.arange(GROUP // block_rows, dtype=jnp.int32))
    return blocks.reshape(GROUP, HEADS, HD)

def layer_group(weights, inputs, seq_lengths, slot_order):
    copies = [low(item) for item in weights]
    gain_one, query_copy, key_copy, value_copy, out_copy, gain_two, gate_copy, up_copy, down_copy = copies
    positions = jnp.arange(GROUP, dtype=jnp.int32)
    seq_ends = jnp.cumsum(seq_lengths).astype(jnp.int32)
    seq_ids = lax.optimization_barrier(jnp.sum((positions[:, None] >= seq_ends[None, :]).astype(jnp.int32), axis=1))
    starts = lax.optimization_barrier(jnp.sum(jnp.where(seq_ends[None, :] <= positions[:, None], seq_lengths[None, :], 0), axis=1))
    within = positions - starts
    slot_pos = within[slot_order]
    inverse = jnp.zeros((GROUP,), jnp.int32).at[slot_order].set(positions)
    normed = low(rms_normed(inputs, gain_one))
    queries = low_back(matmul(normed, query_copy)).reshape(GROUP, HEADS, HD)
    queries = low(rotate_pairs(queries, slot_pos))
    key_rows = low_back(matmul(normed, key_copy))
    key_rows = low(rotate_pairs(key_rows[:, None, :], slot_pos)[:, 0, :])
    value_rows = low(low_back(matmul(normed, value_copy)))
    mixed_rows = attend_group(queries[inverse], key_rows[inverse], value_rows[inverse], seq_ids)
    mixed_rows = mixed_rows[slot_order].reshape(GROUP, HEADS * HD)
    attended = low_back(matmul(mixed_rows, out_copy))
    middle = inputs + attended
    normed_two = low(rms_normed(middle, gain_two))
    gate_act = low_back(matmul(normed_two, gate_copy))
    upward = low_back(matmul(normed_two, up_copy))
    hidden = low(jax.nn.silu(gate_act) * upward)
    output_rows = middle + low_back(matmul(hidden, down_copy))
    return (output_rows, jnp.concatenate([key_rows, value_rows], axis=1))

def whole_layer(weights, inputs, seq_lengths, token_deal):
    grouped = inputs.reshape(GROUPS, GROUP, D)

    def one_group(carry, pieces):
        rows_in, lens_in, order_in = pieces
        result = jax.checkpoint(layer_group)(weights, rows_in, lens_in, order_in)
        return (carry, result)
    _, (outputs, shared) = lax.scan(one_group, jnp.zeros((), jnp.float32), (grouped, seq_lengths, token_deal))
    return (outputs.reshape(TOKENS, D), shared.reshape(TOKENS, 2 * HD))

def reference(layer_input, out_grad, kv_grad, lengths, token_deal, attn_gain, query_weight, key_weight, value_weight, out_weight, mlp_gain, gate_weight, up_weight, down_weight):
    weights = (attn_gain, query_weight, key_weight, value_weight, out_weight, mlp_gain, gate_weight, up_weight, down_weight)

    def forward(params, inputs):
        return whole_layer(params, inputs, lengths, token_deal)
    (output_rows, shared), pullback = jax.vjp(forward, weights, layer_input.astype(jnp.float32))
    grads, input_grad = pullback((out_grad.astype(jnp.float32), kv_grad.astype(jnp.float32)))
    return (output_rows.astype(jnp.bfloat16), input_grad, shared.astype(jnp.bfloat16), grads[0], grads[1], grads[2], grads[3], grads[4], grads[5], grads[6], grads[7], grads[8])
```

```python
import functools

import jax
import jax.numpy as jnp
from jax import lax
from jax.experimental import pallas as pl
from jax.experimental.pallas import tpu as pltpu
from jax.sharding import Mesh, PartitionSpec as P

norm_eps = 1e-05
rope_base = 10000.0
masked_score = -1e30
log2_e = 1.4426950408889634
f32 = jnp.float32
bf = jnp.bfloat16
vmem_bytes = 60 * 1024 * 1024


def mm(left, right, left_dim=1, right_dim=0):
    return lax.dot_general(
        left, right, (((left_dim,), (right_dim,)), ((), ())), preferred_element_type=f32
    )


def core_swap(a):
    return lax.ppermute(a, "core", [(0, 1), (1, 0)])


def row_swap(a, k):
    n = lax.axis_size("row")
    return lax.ppermute(a, "row", [(i, i ^ k) for i in range(n)])


def gather_rows(a):
    n = lax.axis_size("row")
    if n != 4:
        return [a] + [row_swap(a, k) for k in range(1, n)]
    along_x, along_y = row_swap(a, 1), row_swap(a, 2)
    half = a.shape[0] // 2
    corner = jnp.concatenate([row_swap(along_x[:half], 2), row_swap(along_y[half:], 1)], axis=0)
    return [a, along_x, along_y, corner]


def exchange_rows(parts):
    return [parts[0]] + [row_swap(parts[k], k) for k in range(1, len(parts))]


def reduce_rows(parts, wire):
    n = len(parts)
    if n != 4:
        total = parts[0].astype(f32)
        for k in range(1, n):
            total = total + row_swap(parts[k].astype(wire), k).astype(f32)
        return total
    half = parts[0].shape[0] // 2
    low = [p[:half].astype(f32) for p in parts]
    high = [p[half:].astype(f32) for p in parts]
    from_x = row_swap(jnp.stack([low[1], low[3]]).astype(wire), 1).astype(f32)
    from_y = row_swap(jnp.stack([high[2], high[3]]).astype(wire), 2).astype(f32)
    last_y = row_swap((low[2] + from_x[1]).astype(wire), 2).astype(f32)
    last_x = row_swap((high[1] + from_y[1]).astype(wire), 1).astype(f32)
    return jnp.concatenate(
        [low[0] + from_x[0] + last_y, high[0] + from_y[0] + last_x], axis=0
    )


def by_row(pieces, axis=0):
    r = lax.axis_index("row")
    n = len(pieces)
    size = pieces[0].shape[axis]
    shape = list(pieces[0].shape)
    shape[axis] = size * n
    whole = jnp.zeros(shape, pieces[0].dtype)
    for k, piece in enumerate(pieces):
        whole = lax.dynamic_update_slice_in_dim(whole, piece, (r ^ k) * size, axis)
    return whole


def reduce_plane(own_part, other_part, wire):
    n = lax.axis_size("row")
    rows = own_part.shape[0] // n
    both = own_part.astype(f32) + core_swap(other_part).astype(f32)
    return reduce_rows([both[k * rows : (k + 1) * rows] for k in range(n)], wire)


def attend_kernel(scale, tile, n_ref, wq_ref, k_ref, vt_ref, bias_ref, cos_ref, sin_ref,
                  q_ref, qt_ref, mix_ref, mixt_ref, lse_ref, qt_all):
    rows, _, width, block = wq_ref.shape
    head = k_ref.shape[1]
    half = head // 2
    tiles = n_ref.shape[0] // tile
    step = pl.program_id(1)

    @pl.when(step == 0)
    def _():
        q = mm(n_ref[:, :width], wq_ref[0, 0])
        for r in range(1, rows):
            q = q + mm(n_ref[:, r * width : (r + 1) * width], wq_ref[r, 0])
        qt = q.T
        for h in range(block // head):
            first = qt[h * head : h * head + half]
            second = qt[h * head + half : (h + 1) * head]
            turned = jnp.concatenate(
                [
                    first * cos_ref[...] - second * sin_ref[...],
                    second * cos_ref[...] + first * sin_ref[...],
                ],
                axis=0,
            )
            qt_ref[h * head : (h + 1) * head, :] = turned.astype(bf)
            q_ref[:, h * head : (h + 1) * head] = turned.T.astype(bf)
            for i in range(tiles):
                qt_all[h * tiles + i] = turned[:, i * tile : (i + 1) * tile].astype(bf)

    for i in range(tiles):
        for h in range(block // head):

            @pl.when(step == h * tiles + i)
            def _(h=h, i=i):
                cols = slice(i * tile, (i + 1) * tile)
                spots = slice(h * head, (h + 1) * head)
                scores = mm(k_ref[...], qt_all[h * tiles + i]) * (scale * log2_e) + bias_ref[:, cols]
                highest = jnp.max(scores, axis=0, keepdims=True)
                weights = jnp.exp2(scores - highest)
                total = jnp.sum(weights, axis=0, keepdims=True)
                mixed = mm(vt_ref[...], weights.astype(bf)) / total
                mixt_ref[spots, cols] = mixed.astype(bf)
                mix_ref[cols, spots] = mixed.T.astype(bf)
                lse_ref[0, h : h + 1, cols] = highest + jnp.log2(total)


def attend(normed, wq, keys, values_t, bias, cosine_t, sine_t, tile):
    rows, blocks, width, block = wq.shape
    tokens, dim = normed.shape
    head = keys.shape[1]
    heads = block // head
    whole = lambda a: pl.BlockSpec(a.shape, lambda z, j: (0,) * a.ndim)
    return pl.pallas_call(
        functools.partial(attend_kernel, head**-0.5, tile),
        grid=(blocks, heads * (tokens // tile)),
        in_specs=[
            whole(normed),
            pl.BlockSpec((rows, 1, width, block), lambda z, j: (0, z, 0, 0)),
            whole(keys),
            whole(values_t),
            whole(bias),
            whole(cosine_t),
            whole(sine_t),
        ],
        out_specs=[
            pl.BlockSpec((tokens, block), lambda z, j: (0, z)),
            pl.BlockSpec((block, tokens), lambda z, j: (z, 0)),
            pl.BlockSpec((tokens, block), lambda z, j: (0, z)),
            pl.BlockSpec((block, tokens), lambda z, j: (z, 0)),
            pl.BlockSpec((1, heads, tokens), lambda z, j: (z, 0, 0)),
        ],
        out_shape=[
            jax.ShapeDtypeStruct((tokens, blocks * block), bf),
            jax.ShapeDtypeStruct((blocks * block, tokens), bf),
            jax.ShapeDtypeStruct((tokens, blocks * block), bf),
            jax.ShapeDtypeStruct((blocks * block, tokens), bf),
            jax.ShapeDtypeStruct((blocks, heads, tokens), f32),
        ],
        scratch_shapes=[pltpu.VMEM((heads * (tokens // tile), head, tile), bf)],
        compiler_params=pltpu.CompilerParams(vmem_limit_bytes=vmem_bytes),
        cost_estimate=pl.CostEstimate(
            flops=2 * tokens * blocks * block * (dim + 2 * keys.shape[0]),
            bytes_accessed=16 << 20,
            transcendentals=tokens * blocks * heads * keys.shape[0],
        ),
        name="attend",
    )(normed, wq, keys, values_t, bias, cosine_t, sine_t)


def out_kernel(own, m_ref, w_ref, own_ref, other_ref):
    full = mm(m_ref[...], w_ref[0])
    own_ref[...] = full[:own]
    other_ref[...] = full[own:]


def out_project(mixed, wo, own):
    rows, depth, width = wo.shape
    tokens = mixed.shape[0]
    return pl.pallas_call(
        functools.partial(out_kernel, own),
        grid=(rows,),
        in_specs=[
            pl.BlockSpec((tokens, depth), lambda r: (0, 0)),
            pl.BlockSpec((1, depth, width), lambda r: (r, 0, 0)),
        ],
        out_specs=[
            pl.BlockSpec((own, width), lambda r: (0, r)),
            pl.BlockSpec((tokens - own, width), lambda r: (0, r)),
        ],
        out_shape=[
            jax.ShapeDtypeStruct((own, rows * width), f32),
            jax.ShapeDtypeStruct((tokens - own, rows * width), f32),
        ],
        compiler_params=pltpu.CompilerParams(vmem_limit_bytes=vmem_bytes),
        cost_estimate=pl.CostEstimate(
            flops=2 * tokens * depth * rows * width, bytes_accessed=10 << 20, transcendentals=0
        ),
        name="out_project",
    )(mixed, wo)


def attend_back_kernel(scale, tile, ml_ref, wo_ref, wq_ref, nt_ref, k_ref, kt_ref, v_ref, bias_ref,
                       cos_ref, sin_ref, q_ref, qt_ref, mixt_ref, lse_ref,
                       dwq_ref, dwo_ref, dn_ref, dk_ref, dv_ref, do_all, dot_all, dq_all):
    rows, _, width, block = wq_ref.shape
    head = k_ref.shape[1]
    half = head // 2
    tiles = ml_ref.shape[0] // tile
    heads = block // head
    step = pl.program_id(1)

    @pl.when((pl.program_id(0) == 0) & (step == 0))
    def _():
        dk_ref[...] = jnp.zeros_like(dk_ref)
        dv_ref[...] = jnp.zeros_like(dv_ref)
        dn_ref[...] = jnp.zeros_like(dn_ref)

    @pl.when(step == 0)
    def _():
        grad = mm(ml_ref[:, :width], wo_ref[0, 0], 1, 1)
        for r in range(1, rows):
            grad = grad + mm(ml_ref[:, r * width : (r + 1) * width], wo_ref[r, 0], 1, 1)
        grad_t = grad.T
        do_all[...] = grad.astype(bf)
        dot_all[...] = grad_t.astype(bf)

    for i in range(tiles):
        for h in range(heads):

            @pl.when(step == h * tiles + i)
            def _(h=h, i=i):
                cols = slice(i * tile, (i + 1) * tile)
                spots = slice(h * head, (h + 1) * head)
                scores = mm(k_ref[...], qt_ref[spots, cols]) * (scale * log2_e) + bias_ref[:, cols]
                soft = jnp.exp2(scores - lse_ref[0, h : h + 1, cols])
                prob_grad = mm(v_ref[...], dot_all[spots, cols])
                row_dot = jnp.sum(soft * prob_grad, axis=0, keepdims=True)
                score_grad = (soft * (prob_grad - row_dot)).astype(bf)
                dv_ref[...] += mm(soft.astype(bf), do_all[cols, spots])
                dk_ref[...] += mm(score_grad, q_ref[cols, spots]) * scale
                dqt = mm(kt_ref[...], score_grad) * scale
                first, second = dqt[:half], dqt[half:]
                cosine, sine = cos_ref[:, cols], sin_ref[:, cols]
                turned = jnp.concatenate(
                    [first * cosine + second * sine, second * cosine - first * sine], axis=0
                )
                dq_all[cols, spots] = turned.T.astype(bf)

    @pl.when(step == tiles * heads - 1)
    def _():
        dq = dq_all[...]
        for r in range(rows):
            span = slice(r * width, (r + 1) * width)
            dwq_ref[r, 0] = mm(nt_ref[span, :], dq).astype(bf)
            dwo_ref[r, 0] = mm(mixt_ref[...], ml_ref[:, span]).astype(bf)
            dn_ref[:, span] += mm(dq, wq_ref[r, 0], 1, 1)


def attend_back(middle_low, wo, wq, normed_t, keys, keys_t, values, bias, cosine_t, sine_t,
                q, qt, mixed_t, lse, tile):
    rows, blocks, width, block = wq.shape
    tokens, dim = middle_low.shape
    keys_in, head = keys.shape
    heads = block // head
    whole = lambda a: pl.BlockSpec(a.shape, lambda z, j: (0,) * a.ndim)
    return pl.pallas_call(
        functools.partial(attend_back_kernel, head**-0.5, tile),
        grid=(blocks, heads * (tokens // tile)),
        in_specs=[
            whole(middle_low),
            pl.BlockSpec((rows, 1, block, width), lambda z, j: (0, z, 0, 0)),
            pl.BlockSpec((rows, 1, width, block), lambda z, j: (0, z, 0, 0)),
            whole(normed_t),
            whole(keys),
            whole(keys_t),
            whole(values),
            whole(bias),
            whole(cosine_t),
            whole(sine_t),
            pl.BlockSpec((tokens, block), lambda z, j: (0, z)),
            pl.BlockSpec((block, tokens), lambda z, j: (z, 0)),
            pl.BlockSpec((block, tokens), lambda z, j: (z, 0)),
            pl.BlockSpec((1, heads, tokens), lambda z, j: (z, 0, 0)),
        ],
        out_specs=[
            pl.BlockSpec((rows, 1, width, block), lambda z, j: (0, z, 0, 0)),
            pl.BlockSpec((rows, 1, block, width), lambda z, j: (0, z, 0, 0)),
            pl.BlockSpec((tokens, dim), lambda z, j: (0, 0)),
            pl.BlockSpec((keys_in, head), lambda z, j: (0, 0)),
            pl.BlockSpec((keys_in, head), lambda z, j: (0, 0)),
        ],
        out_shape=[
            jax.ShapeDtypeStruct((rows, blocks, width, block), bf),
            jax.ShapeDtypeStruct((rows, blocks, block, width), bf),
            jax.ShapeDtypeStruct((tokens, dim), f32),
            jax.ShapeDtypeStruct((keys_in, head), f32),
            jax.ShapeDtypeStruct((keys_in, head), f32),
        ],
        scratch_shapes=[
            pltpu.VMEM((tokens, block), bf),
            pltpu.VMEM((block, tokens), bf),
            pltpu.VMEM((tokens, block), bf),
        ],
        compiler_params=pltpu.CompilerParams(vmem_limit_bytes=vmem_bytes),
        cost_estimate=pl.CostEstimate(
            flops=2 * tokens * blocks * block * (4 * dim + 5 * keys_in),
            bytes_accessed=32 << 20,
            transcendentals=tokens * blocks * heads * keys_in,
        ),
        name="attend_back",
    )(middle_low, wo, wq, normed_t, keys, keys_t, values, bias, cosine_t, sine_t, q, qt, mixed_t, lse)


def mlp_kernel(x_ref, g_ref, gate_ref, up_ref, down_ref, hid_ref, gg_ref, ug_ref, dx_ref):
    gate = mm(x_ref[...], gate_ref[...], 1, 1)
    up = mm(x_ref[...], up_ref[...], 1, 1)
    hidden_grad = mm(g_ref[...], down_ref[...], 1, 1)
    sig = jax.nn.sigmoid(gate)
    silu = gate * sig
    hid_ref[...] = (silu * up).astype(bf)
    gate_grad = (hidden_grad * up * sig * (1.0 + gate * (1.0 - sig))).astype(bf)
    up_grad = (hidden_grad * silu).astype(bf)
    gg_ref[...] = gate_grad
    ug_ref[...] = up_grad
    dx_ref[...] = (mm(gate_grad, gate_ref[...]) + mm(up_grad, up_ref[...])).astype(bf)


def mlp(x, g, gate_w, up_w, down_w, tile):
    tokens, dim = x.shape
    units = gate_w.shape[0]
    rows_of = lambda width: pl.BlockSpec((tile, width), lambda t: (t, 0))
    weight = pl.BlockSpec((units, dim), lambda t: (0, 0))
    return pl.pallas_call(
        mlp_kernel,
        grid=(tokens // tile,),
        in_specs=[rows_of(dim), rows_of(dim), weight, weight, weight],
        out_specs=[rows_of(units), rows_of(units), rows_of(units), rows_of(dim)],
        out_shape=[jax.ShapeDtypeStruct((tokens, units), bf)] * 3
        + [jax.ShapeDtypeStruct((tokens, dim), bf)],
        compiler_params=pltpu.CompilerParams(vmem_limit_bytes=vmem_bytes),
        cost_estimate=pl.CostEstimate(
            flops=10 * tokens * units * dim, bytes_accessed=24 << 20, transcendentals=tokens * units
        ),
        name="mlp",
    )(x, g, gate_w, up_w, down_w)


def rotate(values, cosine, sine):
    half = values.shape[1] // 2
    first, second = values[:, :half], values[:, half:]
    return jnp.concatenate([first * cosine - second * sine, second * cosine + first * sine], axis=1)


def norm_backward(values, factor, gain, grad_rows):
    weighted = grad_rows * gain
    inner_mean = jnp.mean(weighted * values, axis=-1, keepdims=True)
    input_part = factor * weighted - values * factor * factor * factor * inner_mean
    gain_part = jnp.sum(grad_rows * values * factor, axis=0)
    return (input_part, gain_part)


def local(layer_input, out_grad, kv_grad, lengths, token_deal, attn_gain, query_weight, key_weight,
          value_weight, out_weight, mlp_gain, gate_weight, up_weight, down_weight):
    r, z, c = lax.axis_index("row"), lax.axis_index("z"), lax.axis_index("core")
    n_rows, n_z = lax.axis_size("row"), lax.axis_size("z")
    own, dim = layer_input.shape
    width, block = query_weight.shape
    head = key_weight.shape[1]
    units = gate_weight.shape[1]
    piece = units // n_rows
    pick = lambda a, i, axis=0: lax.dynamic_index_in_dim(a, i, axis, keepdims=False)
    first_core = c == 0

    wq_z = lax.all_gather(query_weight.astype(bf), "z", axis=0)
    wo_z = lax.all_gather(out_weight.astype(bf), "z", axis=0)
    mlp_own = jnp.stack(
        [gate_weight.astype(bf).T, up_weight.astype(bf).T, down_weight.astype(bf)]
    ).reshape(3, n_rows, piece, width)
    mlp_parts = by_row(exchange_rows([pick(mlp_own, r ^ k, 1) for k in range(n_rows)]), axis=2)
    gate_w, up_w, down_w = [
        lax.all_gather(mlp_parts[i], "z", axis=0).reshape(n_z * piece, dim) for i in range(3)
    ]
    gains = jnp.concatenate([attn_gain, mlp_gain]).astype(bf).reshape(-1, head)
    small = jnp.concatenate([jnp.where(first_core, key_weight, value_weight).astype(bf), gains])
    small = by_row(exchange_rows([small] * n_rows)).reshape(n_rows, -1, head)
    kv_w = small[:, :width].reshape(dim, head)
    gains = small[:, width:].reshape(n_rows, 2, width).astype(f32)
    gain_one, gain_two = gains[:, 0].reshape(dim), gains[:, 1].reshape(dim)

    chip = 2 * own
    deal = token_deal[0]
    ends = jnp.cumsum(lengths[0])

    def start_of(initial):
        return jnp.sum(jnp.where(ends[None, :] <= initial[:, None], lengths[0][None, :], 0), axis=1)

    chip_slots = lax.dynamic_slice_in_dim(deal, z * chip, chip, 0)
    swap_halves = lambda a: jnp.where(first_core, a, jnp.roll(a, own, axis=0))
    initial = swap_halves(chip_slots)
    start = start_of(initial)
    angles = (initial - start).astype(f32)[:, None] * (
        rope_base ** (-jnp.arange(head // 2, dtype=f32) / (head // 2))
    )
    cosine, sine = jnp.cos(angles), jnp.sin(angles)
    bias = jnp.where(
        (deal[:, None] >= start[None, :]) & (deal[:, None] <= initial[None, :]), 0.0, masked_score
    ).astype(f32)
    kv_cosine, kv_sine = jnp.where(first_core, cosine, 1.0), jnp.where(first_core, sine, 0.0)

    chip_input = jnp.concatenate([layer_input, core_swap(layer_input)]).astype(f32)
    factor_chip = lax.rsqrt(jnp.mean(chip_input * chip_input, axis=-1, keepdims=True) + norm_eps)
    normed = (chip_input * factor_chip * gain_one).astype(bf)
    input_rows, factor_one = chip_input[:own], factor_chip[:own]
    kv_own = swap_halves(rotate(mm(normed, kv_w), kv_cosine, kv_sine).astype(bf))
    kv_mine = lax.all_gather(kv_own, "z", axis=0, tiled=True)
    kv_other = core_swap(kv_mine)
    keys = jnp.where(first_core, kv_mine, kv_other)
    values = jnp.where(first_core, kv_other, kv_mine)
    shared_own = lax.dynamic_slice_in_dim(
        jnp.concatenate([keys, values], axis=1), (2 * z + c) * own, own, 0
    )

    wq = by_row([a[None] for a in gather_rows(wq_z)])
    wo = by_row([a[None] for a in gather_rows(wo_z)])
    tile = own
    q, qt, mixed, mixed_t, lse = attend(
        normed, wq, keys, values.T, bias, cosine.T, sine.T, tile
    )
    att_own, att_other = out_project(mixed, wo.reshape(n_rows, n_z * block, width), own)
    middle = input_rows + (att_own + core_swap(att_other))
    factor_two = lax.rsqrt(jnp.mean(middle * middle, axis=-1, keepdims=True) + norm_eps)
    normed_two = (middle * factor_two * gain_two).astype(bf)

    grads_own = jnp.concatenate(gather_rows(out_grad))
    grads_other = core_swap(grads_own)
    rows_own = jnp.concatenate(gather_rows(normed_two))
    rows_other = core_swap(rows_own)
    hid_a, gg_a, ug_a, dx_a = mlp(rows_own, grads_own, gate_w, up_w, down_w, own)
    hid_b, gg_b, ug_b, dx_b = mlp(rows_other, grads_other, gate_w, up_w, down_w, own)
    normed_two_grad = reduce_plane(dx_a, dx_b, bf)
    down_part = (mm(hid_a, grads_own, 0, 0) + mm(hid_b, grads_other, 0, 0)).astype(bf)
    gate_part = (mm(gg_a, rows_own, 0, 0) + mm(gg_b, rows_other, 0, 0)).astype(bf)
    up_part = (mm(ug_a, rows_own, 0, 0) + mm(ug_b, rows_other, 0, 0)).astype(bf)
    output_rows = middle + reduce_plane(
        mm(hid_a, down_w).astype(bf), mm(hid_b, down_w).astype(bf), bf
    )
    mlp_sums = jnp.stack(
        [
            lax.psum_scatter(a, "z", scatter_dimension=0, tiled=True)
            for a in (gate_part, up_part, down_part)
        ]
    ).reshape(3, piece, n_rows, width)
    mlp_grads = by_row(exchange_rows([pick(mlp_sums, r ^ k, 2) for k in range(n_rows)]), axis=1)
    mlp_grads = mlp_grads.astype(f32)

    middle_part, gain_two_grad = norm_backward(middle, factor_two, gain_two, normed_two_grad)
    middle_grad = out_grad.astype(f32) + middle_part
    low_own = middle_grad.astype(bf)
    middle_low = jnp.concatenate([low_own, core_swap(low_own)])

    dwq, dwo, dn, dk, dv = attend_back(
        middle_low, wo, wq, normed.T, keys, keys.T, values, bias, cosine.T, sine.T,
        q, qt, mixed_t, lse, tile,
    )
    dwo_rows = reduce_rows([pick(dwo, r ^ k) for k in range(n_rows)], bf).astype(bf)
    dwq_rows = reduce_rows([pick(dwq, r ^ k) for k in range(n_rows)], bf).astype(bf)
    out_wgrad = lax.psum_scatter(dwo_rows, "z", scatter_dimension=0, tiled=False).astype(f32)
    query_wgrad = lax.psum_scatter(dwq_rows, "z", scatter_dimension=0, tiled=False).astype(f32)

    kv_sum = jnp.where(first_core, dk, dv) + core_swap(jnp.where(first_core, dv, dk))
    kv_sum = lax.all_to_all(
        kv_sum.astype(bf).reshape(n_z, chip, head), "z", split_axis=0, concat_axis=0, tiled=False
    )
    kv_grad32 = kv_grad.astype(f32)
    kv_left, kv_right = kv_grad[:, :head], kv_grad[:, head:]
    kv_given = jnp.concatenate(
        [
            jnp.where(first_core, kv_left, kv_right),
            core_swap(jnp.where(first_core, kv_right, kv_left)),
        ]
    ).astype(f32)
    kv_sum = swap_halves(jnp.sum(kv_sum.astype(f32), axis=0)) + kv_given
    kv_low = rotate(kv_sum, kv_cosine, -kv_sine).astype(bf)
    kv_wgrad = mm(normed, kv_low, 0, 0)
    dn = dn + mm(kv_low, kv_w, 1, 1)
    normed_one_grad = dn[:own] + core_swap(dn[own:])
    input_part, gain_one_grad = norm_backward(input_rows, factor_one, gain_one, normed_one_grad)
    input_grad = middle_grad + input_part

    gain_rows = jnp.stack(
        [gain_one_grad.reshape(n_rows, width), gain_two_grad.reshape(n_rows, width)], axis=1
    ).reshape(n_rows, -1, head)
    small = jnp.concatenate([kv_wgrad.reshape(n_rows, width, head), gain_rows], axis=1)
    small = reduce_rows([pick(small, r ^ k) for k in range(n_rows)], f32)
    k = 1
    while k < n_z:
        small = small + lax.ppermute(small, "z", [(i, i ^ k) for i in range(n_z)])
        k *= 2
    small_other = core_swap(small)
    key_wgrad = jnp.where(first_core, small[:width], small_other[:width])
    value_wgrad = jnp.where(first_core, small_other[:width], small[:width])
    gain_sums = (small[width:] + small_other[width:]).reshape(2, width)
    return (
        output_rows.astype(bf),
        input_grad,
        shared_own,
        gain_sums[0],
        query_wgrad,
        key_wgrad,
        value_wgrad,
        out_wgrad,
        gain_sums[1],
        mlp_grads[0].T,
        mlp_grads[1].T,
        mlp_grads[2],
    )


def solution(mesh):
    n_rows, n_cols = mesh.shape["row"], mesh.shape["col"]
    split = Mesh(mesh.devices.reshape(n_rows, n_cols // 2, 2), ("row", "z", "core"))
    everywhere, col = ("row", "z", "core"), ("z", "core")
    in_specs = (
        P(everywhere, None),
        P(everywhere, None),
        P(everywhere, None),
        P("row", None),
        P("row", None),
        P("row"),
        P("row", col),
        P("row", None),
        P("row", None),
        P(col, "row"),
        P("row"),
        P("row", col),
        P("row", col),
        P(col, "row"),
    )
    out_specs = (
        P(everywhere, None),
        P(everywhere, None),
        P(everywhere, None),
        P("row"),
        P("row", col),
        P("row", None),
        P("row", None),
        P(col, "row"),
        P("row"),
        P("row", col),
        P("row", col),
        P(col, "row"),
    )
    return jax.shard_map(
        local, mesh=split, in_specs=in_specs, out_specs=out_specs, check_vma=False
    )
```

```python
import functools

import jax
import jax.numpy as jnp
from jax import lax
from jax.experimental import pallas as pl
from jax.experimental.pallas import tpu as pltpu
from jax.sharding import Mesh, PartitionSpec as P

norm_eps = 1e-05
rope_base = 10000.0
masked_score = -1e30
log2_e = 1.4426950408889634
f32 = jnp.float32
bf = jnp.bfloat16
vmem_bytes = 60 * 1024 * 1024


def mm(left, right, left_dim=1, right_dim=0):
    return lax.dot_general(
        left, right, (((left_dim,), (right_dim,)), ((), ())), preferred_element_type=f32
    )


def core_swap(a):
    return lax.ppermute(a, "core", [(0, 1), (1, 0)])


def axis_swap(a, axis, k):
    return lax.ppermute(a, axis, [(i, i ^ k) for i in range(lax.axis_size(axis))])


def row_swap(a, k):
    return axis_swap(a, "row", k)


def after(values, earlier):
    return lax.optimization_barrier((values, earlier))[0]


def gather_rows(a, cover=()):
    n = lax.axis_size("row")
    if n != 4:
        return [a] + [row_swap(a, k) for k in range(1, n)], cover
    along_x, along_y, cover = lax.optimization_barrier((row_swap(a, 1), row_swap(a, 2), cover))
    half = a.shape[0] // 2
    corner = jnp.concatenate([row_swap(along_x[:half], 2), row_swap(along_y[half:], 1)], axis=0)
    return [a, along_x, along_y, corner], cover


def exchange_rows(parts):
    return [parts[0]] + [row_swap(parts[k], k) for k in range(1, len(parts))]


def part_sum(parts, k, cut=slice(None)):
    return sum(term[cut].astype(f32) for term in parts[k])


def halves_of(parts):
    half = parts[0][0].shape[0] // 2
    return slice(0, half), slice(half, None)


def row_messages(parts):
    n = len(parts)
    if n != 4:
        return tuple(part_sum(parts, k).astype(bf) for k in range(1, n))
    low, high = halves_of(parts)
    return (
        jnp.stack([part_sum(parts, 1, low), part_sum(parts, 3, low)]).astype(bf),
        jnp.stack([part_sum(parts, 2, high), part_sum(parts, 3, high)]).astype(bf),
    )


def swap_first(messages):
    return tuple(row_swap(message, k) for k, message in enumerate(messages, 1))


def row_turned(parts, received):
    if len(parts) != 4:
        return ()
    low, high = halves_of(parts)
    from_x, from_y = received
    return (
        (part_sum(parts, 1, high) + from_y[1].astype(f32)).astype(bf),
        (part_sum(parts, 2, low) + from_x[1].astype(f32)).astype(bf),
    )


def row_total(parts, received, last):
    if len(parts) != 4:
        return part_sum(parts, 0) + sum(a.astype(f32) for a in received)
    from_x, from_y = received
    last_x, last_y = last
    first = jnp.concatenate([from_x[0], from_y[0]]).astype(f32)
    return part_sum(parts, 0) + first + jnp.concatenate([last_y, last_x]).astype(f32)


def by_row(pieces, axis=0):
    r = lax.axis_index("row")
    size = pieces[0].shape[axis]
    shape = list(pieces[0].shape)
    shape[axis] = size * len(pieces)
    whole = jnp.zeros(shape, pieces[0].dtype)
    for k, piece in enumerate(pieces):
        whole = lax.dynamic_update_slice_in_dim(whole, piece, (r ^ k) * size, axis)
    return whole


def reduce_z(a):
    n, z = lax.axis_size("z"), lax.axis_index("z")
    size = a.shape[0] // n
    a = jnp.concatenate([lax.dynamic_slice_in_dim(a, (z ^ k) * size, size, 0) for k in range(n)])
    k = n // 2
    while k >= 1:
        half = a.shape[0] // 2
        a = a[:half] + axis_swap(a[half:].astype(bf), "z", k).astype(f32)
        k //= 2
    return a


def row_parts(total, rows):
    return [total[k * rows : (k + 1) * rows] for k in range(total.shape[0] // rows)]


def call(kernel, out_shape, name, flops, bytes_moved, transcendentals=0, **more):
    return pl.pallas_call(
        kernel,
        out_shape=out_shape,
        compiler_params=pltpu.CompilerParams(vmem_limit_bytes=vmem_bytes),
        cost_estimate=pl.CostEstimate(
            flops=flops, bytes_accessed=bytes_moved, transcendentals=transcendentals
        ),
        name=name,
        **more,
    )


def span_of(k, width):
    return pl.ds(pl.multiple_of((lax.axis_index("row") ^ k) * width, 128), width)


def scale_of(values):
    return lax.rsqrt(jnp.mean(values * values, axis=-1, keepdims=True) + norm_eps)


def norm_one_kernel(a_ref, b_ref, gain_ref, out_ref):
    own = a_ref.shape[0]
    for i, ref in enumerate((a_ref, b_ref)):
        values = ref[...].astype(f32)
        out_ref[i * own : (i + 1) * own, :] = (values * scale_of(values) * gain_ref[...]).astype(bf)


def norm_one(a, b, gain):
    own, dim = a.shape
    return call(
        norm_one_kernel, jax.ShapeDtypeStruct((2 * own, dim), bf), "norm_one", 8 * own * dim, 8 * own * dim
    )(a, b, gain)


def norm_two_kernel(x_ref, a_ref, b_ref, gain_ref, middle_ref, out_ref):
    middle = x_ref[...].astype(f32) + (a_ref[...] + b_ref[...])
    middle_ref[...] = middle
    out_ref[...] = (middle * scale_of(middle) * gain_ref[...]).astype(bf)


def norm_two(x, a, b, gain):
    own, dim = x.shape
    return call(
        norm_two_kernel,
        [jax.ShapeDtypeStruct((own, dim), f32), jax.ShapeDtypeStruct((own, dim), bf)],
        "norm_two",
        8 * own * dim,
        16 * own * dim,
    )(x, a, b, gain)


def through_norm(values, gain, grad):
    factor = scale_of(values)
    weighted = grad * gain
    inner = jnp.mean(weighted * values, axis=-1, keepdims=True)
    gain_part = jnp.sum(grad * values * factor, axis=0, keepdims=True)
    return factor * weighted - values * (factor * factor * factor * inner), gain_part


def norm_two_back_kernel(middle_ref, grad_ref, out_grad_ref, gain_ref, sum_ref, low_ref, gain_grad_ref):
    part, gain_grad_ref[...] = through_norm(middle_ref[...], gain_ref[...], grad_ref[...])
    total = out_grad_ref[...].astype(f32) + part
    sum_ref[...] = total
    low_ref[...] = total.astype(bf)


def norm_two_back(middle, grad, out_grad, gain):
    own, dim = middle.shape
    return call(
        norm_two_back_kernel,
        [
            jax.ShapeDtypeStruct((own, dim), f32),
            jax.ShapeDtypeStruct((own, dim), bf),
            jax.ShapeDtypeStruct((1, dim), f32),
        ],
        "norm_two_back",
        16 * own * dim,
        16 * own * dim,
    )(middle, grad, out_grad, gain)


def norm_one_back_kernel(x_ref, a_ref, b_ref, gain_ref, sum_ref, out_ref, gain_grad_ref):
    part, gain_grad_ref[...] = through_norm(
        x_ref[...].astype(f32), gain_ref[...], a_ref[...] + b_ref[...]
    )
    out_ref[...] = sum_ref[...] + part


def norm_one_back(x, a, b, gain, middle_grad):
    own, dim = x.shape
    return call(
        norm_one_back_kernel,
        [jax.ShapeDtypeStruct((own, dim), f32), jax.ShapeDtypeStruct((1, dim), f32)],
        "norm_one_back",
        16 * own * dim,
        18 * own * dim,
    )(x, a, b, gain, middle_grad)


def attend_kernel(scale, tile, rows, *refs):
    n_ref, wq_refs = refs[0], refs[1 : 1 + rows]
    k_ref, vt_ref, bias_ref, cos_ref, sin_ref = refs[1 + rows : 6 + rows]
    q_ref, qt_ref, mix_ref, lse_ref, qt_all = refs[6 + rows :]
    _, width, block = wq_refs[0].shape
    head = k_ref.shape[1]
    half = head // 2
    tiles = n_ref.shape[0] // tile
    step = pl.program_id(1)

    @pl.when(step == 0)
    def _():
        q = mm(n_ref[:, span_of(0, width)], wq_refs[0][0])
        for k in range(1, rows):
            q = q + mm(n_ref[:, span_of(k, width)], wq_refs[k][0])
        qt = q.T
        for h in range(block // head):
            first = qt[h * head : h * head + half]
            second = qt[h * head + half : (h + 1) * head]
            turned = jnp.concatenate(
                [
                    first * cos_ref[...] - second * sin_ref[...],
                    second * cos_ref[...] + first * sin_ref[...],
                ],
                axis=0,
            )
            qt_ref[h * head : (h + 1) * head, :] = turned.astype(bf)
            q_ref[:, h * head : (h + 1) * head] = turned.T.astype(bf)
            for i in range(tiles):
                qt_all[h * tiles + i] = turned[:, i * tile : (i + 1) * tile].astype(bf)

    for i in range(tiles):
        for h in range(block // head):

            @pl.when(step == h * tiles + i)
            def _(h=h, i=i):
                cols = slice(i * tile, (i + 1) * tile)
                spots = slice(h * head, (h + 1) * head)
                scores = mm(k_ref[...], qt_all[h * tiles + i]) * (scale * log2_e) + bias_ref[:, cols]
                highest = jnp.max(scores, axis=0, keepdims=True)
                weights = jnp.exp2(scores - highest)
                total = jnp.sum(weights, axis=0, keepdims=True)
                mixed = mm(vt_ref[...], weights.astype(bf)) / total
                mix_ref[cols, spots] = mixed.T.astype(bf)
                lse_ref[0, h : h + 1, cols] = highest + jnp.log2(total)


def full_spec(a):
    return pl.BlockSpec(a.shape, lambda *_: (0,) * a.ndim)


def attend(normed, wq, keys, values_t, bias, cosine_t, sine_t, tile):
    rows = len(wq)
    blocks, width, block = wq[0].shape
    tokens, dim = normed.shape
    head = keys.shape[1]
    heads = block // head
    small = (keys, values_t, bias, cosine_t, sine_t)
    return call(
        functools.partial(attend_kernel, head**-0.5, tile, rows),
        [
            jax.ShapeDtypeStruct((tokens, blocks * block), bf),
            jax.ShapeDtypeStruct((blocks * block, tokens), bf),
            jax.ShapeDtypeStruct((tokens, blocks * block), bf),
            jax.ShapeDtypeStruct((blocks, heads, tokens), f32),
        ],
        "attend",
        2 * tokens * blocks * block * (dim + 2 * keys.shape[0]),
        16 << 20,
        tokens * blocks * heads * keys.shape[0],
        grid=(blocks, heads * (tokens // tile)),
        in_specs=[full_spec(normed)]
        + [pl.BlockSpec((1, width, block), lambda z, j: (z, 0, 0))] * rows
        + [full_spec(a) for a in small],
        out_specs=[
            pl.BlockSpec((tokens, block), lambda z, j: (0, z)),
            pl.BlockSpec((block, tokens), lambda z, j: (z, 0)),
            pl.BlockSpec((tokens, block), lambda z, j: (0, z)),
            pl.BlockSpec((1, heads, tokens), lambda z, j: (z, 0, 0)),
        ],
        scratch_shapes=[pltpu.VMEM((heads * (tokens // tile), head, tile), bf)],
    )(normed, *wq, *small)


def out_kernel(own, rows, m_ref, *refs):
    wo_refs, own_ref, other_ref = refs[:rows], refs[rows], refs[rows + 1]
    _, width, block = wo_refs[0].shape
    z = pl.program_id(0)
    for k in range(rows):
        part = mm(m_ref[...], wo_refs[k][0], 1, 1)
        for ref, rest in ((own_ref, part[:own]), (other_ref, part[own:])):
            span = span_of(k, width)

            @pl.when(z == 0)
            def _():
                ref[:, span] = rest

            @pl.when(z != 0)
            def _():
                ref[:, span] += rest


def out_project(mixed, wo, own):
    rows = len(wo)
    blocks, width, block = wo[0].shape
    tokens = mixed.shape[0]
    out = jax.ShapeDtypeStruct((own, rows * width), f32)
    return call(
        functools.partial(out_kernel, own, rows),
        [out, out],
        "out_project",
        2 * tokens * blocks * block * rows * width,
        10 << 20,
        grid=(blocks,),
        in_specs=[pl.BlockSpec((tokens, block), lambda z: (0, z))]
        + [pl.BlockSpec((1, width, block), lambda z: (z, 0, 0))] * rows,
        out_specs=[pl.BlockSpec((own, rows * width), lambda z: (0, 0))] * 2,
    )(mixed, *wo)


def attend_back_kernel(scale, tile, rows, *refs):
    ml_ref, wo_refs = refs[0], refs[1 : 1 + rows]
    (k_ref, kt_ref, v_ref, bias_ref, cos_ref, sin_ref, q_ref, qt_ref, lse_ref) = refs[1 + rows : 10 + rows]
    dq_ref, dk_ref, dv_ref, do_all, dot_all = refs[10 + rows :]
    _, width, block = wo_refs[0].shape
    head = k_ref.shape[1]
    half = head // 2
    tiles = ml_ref.shape[0] // tile
    heads = block // head
    step = pl.program_id(1)

    @pl.when((pl.program_id(0) == 0) & (step == 0))
    def _():
        dk_ref[...] = jnp.zeros_like(dk_ref)
        dv_ref[...] = jnp.zeros_like(dv_ref)

    @pl.when(step == 0)
    def _():
        grad = mm(ml_ref[:, span_of(0, width)], wo_refs[0][0])
        for k in range(1, rows):
            grad = grad + mm(ml_ref[:, span_of(k, width)], wo_refs[k][0])
        do_all[...] = grad.astype(bf)
        dot_all[...] = grad.T.astype(bf)

    for i in range(tiles):
        for h in range(heads):

            @pl.when(step == h * tiles + i)
            def _(h=h, i=i):
                cols = slice(i * tile, (i + 1) * tile)
                spots = slice(h * head, (h + 1) * head)
                scores = mm(k_ref[...], qt_ref[spots, cols]) * (scale * log2_e) + bias_ref[:, cols]
                soft = jnp.exp2(scores - lse_ref[0, h : h + 1, cols])
                prob_grad = mm(v_ref[...], dot_all[spots, cols])
                row_dot = jnp.sum(soft * prob_grad, axis=0, keepdims=True)
                score_grad = (soft * (prob_grad - row_dot)).astype(bf)
                dv_ref[...] += mm(soft.astype(bf), do_all[cols, spots])
                dk_ref[...] += mm(score_grad, q_ref[cols, spots]) * scale
                dqt = mm(kt_ref[...], score_grad) * scale
                first, second = dqt[:half], dqt[half:]
                cosine, sine = cos_ref[:, cols], sin_ref[:, cols]
                turned = jnp.concatenate(
                    [first * cosine + second * sine, second * cosine - first * sine], axis=0
                )
                dq_ref[cols, spots] = turned.T.astype(bf)


def attend_back(middle_low, wo, keys, keys_t, values, bias, cosine_t, sine_t, q, qt, lse, tile):
    rows = len(wo)
    blocks, width, block = wo[0].shape
    tokens, dim = middle_low.shape
    keys_in, head = keys.shape
    heads = block // head
    small = (keys, keys_t, values, bias, cosine_t, sine_t)
    return call(
        functools.partial(attend_back_kernel, head**-0.5, tile, rows),
        [
            jax.ShapeDtypeStruct((tokens, blocks * block), bf),
            jax.ShapeDtypeStruct((keys_in, head), f32),
            jax.ShapeDtypeStruct((keys_in, head), f32),
        ],
        "attend_back",
        2 * tokens * blocks * block * (dim + 5 * keys_in),
        32 << 20,
        tokens * blocks * heads * keys_in,
        grid=(blocks, heads * (tokens // tile)),
        in_specs=[full_spec(middle_low)]
        + [pl.BlockSpec((1, width, block), lambda z, j: (z, 0, 0))] * rows
        + [full_spec(a) for a in small]
        + [
            pl.BlockSpec((tokens, block), lambda z, j: (0, z)),
            pl.BlockSpec((block, tokens), lambda z, j: (z, 0)),
            pl.BlockSpec((1, heads, tokens), lambda z, j: (z, 0, 0)),
        ],
        out_specs=[
            pl.BlockSpec((tokens, block), lambda z, j: (0, z)),
            pl.BlockSpec((keys_in, head), lambda z, j: (0, 0)),
            pl.BlockSpec((keys_in, head), lambda z, j: (0, 0)),
        ],
        scratch_shapes=[pltpu.VMEM((tokens, block), bf), pltpu.VMEM((block, tokens), bf)],
    )(middle_low, *wo, *small, q, qt, lse)


def outer_kernel(rows, width, a_ref, b_ref, out_ref):
    for k in range(rows):
        out_ref[k, 0] = mm(a_ref[:, span_of(k, width)], b_ref[...], 0, 0).astype(bf)


def outer(a, b, rows, blocks):
    tokens, dim = a.shape
    width, block = dim // rows, b.shape[1] // blocks
    return call(
        functools.partial(outer_kernel, rows, width),
        jax.ShapeDtypeStruct((rows, blocks, width, block), bf),
        "outer",
        2 * tokens * dim * b.shape[1],
        8 << 20,
        grid=(blocks,),
        in_specs=[full_spec(a), pl.BlockSpec((tokens, block), lambda z: (0, z))],
        out_specs=pl.BlockSpec((rows, 1, width, block), lambda z: (0, z, 0, 0)),
    )(a, b)


def query_back_kernel(own, rows, n_ref, dq_ref, *refs):
    wq_refs, dw_ref, own_ref, other_ref = refs[:rows], refs[rows], refs[rows + 1], refs[rows + 2]
    _, width, block = wq_refs[0].shape
    z = pl.program_id(0)
    for k in range(rows):
        span = span_of(k, width)
        dw_ref[k, 0] = mm(n_ref[:, span], dq_ref[...], 0, 0).astype(bf)
        part = mm(dq_ref[...], wq_refs[k][0], 1, 1)
        for ref, rest in ((own_ref, part[:own]), (other_ref, part[own:])):

            @pl.when(z == 0)
            def _():
                ref[:, span] = rest

            @pl.when(z != 0)
            def _():
                ref[:, span] += rest


def query_back(normed, dq, wq, own):
    rows = len(wq)
    blocks, width, block = wq[0].shape
    tokens, dim = normed.shape
    out = jax.ShapeDtypeStruct((own, dim), f32)
    return call(
        functools.partial(query_back_kernel, own, rows),
        [jax.ShapeDtypeStruct((rows, blocks, width, block), bf), out, out],
        "query_back",
        4 * tokens * dim * blocks * block,
        16 << 20,
        grid=(blocks,),
        in_specs=[full_spec(normed), pl.BlockSpec((tokens, block), lambda z: (0, z))]
        + [pl.BlockSpec((1, width, block), lambda z: (z, 0, 0))] * rows,
        out_specs=[pl.BlockSpec((rows, 1, width, block), lambda z: (0, z, 0, 0))]
        + [pl.BlockSpec((own, dim), lambda z: (0, 0))] * 2,
    )(normed, dq, *wq)


def fetch(source, target, sems, which):
    copies = []
    units = source.shape[2]
    for z in range(source.shape[0]):
        for slot, i in enumerate(which):
            copies.append(
                pltpu.make_async_copy(
                    source.at[z, i], target.at[slot, pl.ds(z * units, units)], sems.at[z, slot]
                )
            )
    for copy in copies:
        copy.start()
    for copy in copies:
        copy.wait()


def mlp_kernel(added, x_ref, g_ref, w_ref, *refs):
    prior_ref = refs[0] if added else None
    hid_ref, gg_ref, ug_ref, dx_ref, w_all, sems = refs[1:] if added else refs

    @pl.when(pl.program_id(0) == 0)
    def _():
        fetch(w_ref, w_all, sems, (0, 1, 2))

    gate = mm(x_ref[...], w_all[0], 1, 1)
    up = mm(x_ref[...], w_all[1], 1, 1)
    hidden_grad = mm(g_ref[...], w_all[2], 1, 1)
    sig = jax.nn.sigmoid(gate)
    silu = gate * sig
    hid_ref[...] = (silu * up).astype(bf)
    gate_grad = (hidden_grad * up * sig * (1.0 + gate * (1.0 - sig))).astype(bf)
    up_grad = (hidden_grad * silu).astype(bf)
    gg_ref[...] = gate_grad
    ug_ref[...] = up_grad
    dx = mm(gate_grad, w_all[0]) + mm(up_grad, w_all[1])
    if added:
        dx = dx + prior_ref[...].astype(f32)
    dx_ref[...] = dx.astype(bf)


def mlp(x, g, weights, prior, tile):
    tokens, dim = x.shape
    parts, _, few, _ = weights.shape
    units = parts * few
    rows_of = lambda width: pl.BlockSpec((tile, width), lambda t: (t, 0))
    added = prior is not None
    return call(
        functools.partial(mlp_kernel, added),
        [jax.ShapeDtypeStruct((tokens, units), bf)] * 3 + [jax.ShapeDtypeStruct((tokens, dim), bf)],
        "mlp",
        10 * tokens * units * dim,
        24 << 20,
        tokens * units,
        grid=(tokens // tile,),
        in_specs=[rows_of(dim), rows_of(dim), pl.BlockSpec(memory_space=pl.ANY)]
        + [rows_of(dim)] * added,
        out_specs=[rows_of(units), rows_of(units), rows_of(units), rows_of(dim)],
        scratch_shapes=[
            pltpu.VMEM((3, units, dim), bf),
            pltpu.SemaphoreType.DMA((parts, 3)),
        ],
    )(x, g, weights, *([prior] if added else []))


def mlp_weights_kernel(added, tiles, *refs):
    first, second, w_ref = refs[:5], refs[5:10], refs[10]
    priors = refs[11:13] if added else (None, None)
    dw_ref, out_a, out_b, total, down, sems = refs[13:] if added else refs[11:]
    step = pl.program_id(0)

    @pl.when(step == 0)
    def _():
        fetch(w_ref, down, sems, (2,))
        total[...] = jnp.zeros_like(total)

    def body(terms, prior, out):
        x_ref, g_ref, hid_ref, gg_ref, ug_ref = terms
        total[0] += mm(gg_ref[...], x_ref[...], 0, 0)
        total[1] += mm(ug_ref[...], x_ref[...], 0, 0)
        total[2] += mm(hid_ref[...], g_ref[...], 0, 0)
        part = mm(hid_ref[...], down[0])
        if prior is not None:
            part = part + prior[...].astype(f32)
        out[...] = part.astype(bf)

    @pl.when(step < tiles)
    def _():
        body(first, priors[0], out_a)

    @pl.when(step >= tiles)
    def _():
        body(second, priors[1], out_b)

    @pl.when(step == 2 * tiles - 1)
    def _():
        few = dw_ref.shape[2]
        for z in range(dw_ref.shape[0]):
            for i in range(3):
                dw_ref[z, i] = total[i, z * few : (z + 1) * few, :].astype(bf)


def mlp_weights(first, second, weights, priors, tile):
    tokens, dim = first[0].shape
    parts, _, few, _ = weights.shape
    units = parts * few
    tiles = tokens // tile
    added = priors is not None
    early = lambda width: pl.BlockSpec((tile, width), lambda t: (jnp.minimum(t, tiles - 1), 0))
    late = lambda width: pl.BlockSpec((tile, width), lambda t: (jnp.maximum(t - tiles, 0), 0))
    rows = jax.ShapeDtypeStruct((tokens, dim), bf)
    return call(
        functools.partial(mlp_weights_kernel, added, tiles),
        [jax.ShapeDtypeStruct((parts, 3, few, dim), bf), rows, rows],
        "mlp_weights",
        16 * tokens * units * dim,
        32 << 20,
        grid=(2 * tiles,),
        in_specs=[early(dim), early(dim), early(units), early(units), early(units)]
        + [late(dim), late(dim), late(units), late(units), late(units)]
        + [pl.BlockSpec(memory_space=pl.ANY)]
        + [early(dim), late(dim)] * added,
        out_specs=[
            pl.BlockSpec((parts, 3, few, dim), lambda t: (0, 0, 0, 0)),
            early(dim),
            late(dim),
        ],
        scratch_shapes=[
            pltpu.VMEM((3, units, dim), f32),
            pltpu.VMEM((1, units, dim), bf),
            pltpu.SemaphoreType.DMA((parts, 1)),
        ],
    )(*first, *second, weights, *(priors if added else []))


def rotate(values, cosine, sine):
    half = values.shape[1] // 2
    first, second = values[:, :half], values[:, half:]
    return jnp.concatenate([first * cosine - second * sine, second * cosine + first * sine], axis=1)


def local(layer_input, out_grad, kv_grad, lengths, token_deal, attn_gain, query_weight, key_weight,
          value_weight, out_weight, mlp_gain, gate_weight, up_weight, down_weight):
    r, z, c = lax.axis_index("row"), lax.axis_index("z"), lax.axis_index("core")
    n_rows, n_z = lax.axis_size("row"), lax.axis_size("z")
    own, dim = layer_input.shape
    width, block = query_weight.shape
    head = key_weight.shape[1]
    units = gate_weight.shape[1]
    piece = units // n_rows
    pick = lambda a, i, axis=0: lax.dynamic_index_in_dim(a, i, axis, keepdims=False)
    first_core = c == 0

    wq_z = lax.all_gather(query_weight.astype(bf), "z", axis=0)
    mlp_own = jnp.stack(
        [gate_weight.astype(bf).T, up_weight.astype(bf).T, down_weight.astype(bf)]
    ).reshape(3, n_rows, piece, width)
    mlp_parts = exchange_rows([pick(mlp_own, r ^ k, 1) for k in range(n_rows)])
    gains = jnp.concatenate([attn_gain, mlp_gain]).astype(bf).reshape(-1, head)
    small = jnp.concatenate([jnp.where(first_core, key_weight, value_weight).astype(bf), gains])
    small = by_row(exchange_rows([small] * n_rows)).reshape(n_rows, -1, head)
    kv_w = small[:, :width].reshape(dim, head)
    gains = small[:, width:].reshape(n_rows, 2, width).astype(f32)
    gain_one, gain_two = gains[:, 0].reshape(1, dim), gains[:, 1].reshape(1, dim)

    chip = 2 * own
    deal = token_deal[0]
    ends = jnp.cumsum(lengths[0])

    def start_of(initial):
        return jnp.sum(jnp.where(ends[None, :] <= initial[:, None], lengths[0][None, :], 0), axis=1)

    swap_halves = lambda a: jnp.where(first_core, a, jnp.roll(a, own, axis=0))
    initial = swap_halves(lax.dynamic_slice_in_dim(deal, z * chip, chip, 0))
    start = start_of(initial)
    angles = (initial - start).astype(f32)[:, None] * (
        rope_base ** (-jnp.arange(head // 2, dtype=f32) / (head // 2))
    )
    cosine, sine = jnp.cos(angles), jnp.sin(angles)
    bias = jnp.where(
        (deal[:, None] >= start[None, :]) & (deal[:, None] <= initial[None, :]),
        0.0,
        masked_score,
    ).astype(f32)
    kv_cosine, kv_sine = jnp.where(first_core, cosine, 1.0), jnp.where(first_core, sine, 0.0)

    normed = norm_one(layer_input, core_swap(layer_input), gain_one)
    kv_own = swap_halves(rotate(mm(normed, kv_w), kv_cosine, kv_sine).astype(bf))
    mlp_parts = after(mlp_parts, kv_own)
    kv_mine = lax.all_gather(after(kv_own, wq_z), "z", axis=0, tiled=True)
    kv_other = core_swap(kv_mine)
    keys = jnp.where(first_core, kv_mine, kv_other)
    values = jnp.where(first_core, kv_other, kv_mine)
    mine = lambda a: lax.dynamic_slice_in_dim(a, z * chip + c * own, own, 0)
    shared_own = jnp.concatenate([mine(keys), mine(values)], axis=1)

    wo_z = lax.all_gather(after(out_weight.astype(bf).T, kv_mine), "z", axis=0)
    wq_z = after(wq_z, mlp_parts)
    mlp_parts = by_row(mlp_parts, axis=2)
    late_units = piece * 4 // 11
    cuts = [slice(0, piece - late_units), slice(piece - late_units, piece)]
    few = [cut.stop - cut.start for cut in cuts]
    mlp_w = []
    for cut in cuts:
        earlier = mlp_w[-1] if mlp_w else wo_z
        mlp_w.append(lax.all_gather(after(mlp_parts[:, cut], earlier), "z", axis=0))
    aligned = all(n % 16 == 0 for n in few)
    if not aligned:
        mlp_w = [
            w.transpose(1, 0, 2, 3).reshape(1, 3, n_z * n, dim) for w, n in zip(mlp_w, few)
        ]

    wq, _ = gather_rows(wq_z)
    wo_z = after(wo_z, wq)
    tile = own
    attended = attend(normed, wq, keys, values.T, bias, cosine.T, sine.T, tile)
    wo, (q, qt, mixed, lse) = gather_rows(wo_z, attended)
    att_own, att_other = out_project(mixed, wo, own)
    middle, normed_two = norm_two(layer_input, att_own, core_swap(att_other), gain_two)

    grads_own, normed_two = gather_rows(after(out_grad, wo[3]), normed_two)
    grads_own = jnp.concatenate(grads_own)
    grads_other = core_swap(grads_own)
    rows_own = jnp.concatenate(gather_rows(normed_two)[0])
    rows_other = core_swap(rows_own)
    early_b = mlp(rows_other, grads_other, mlp_w[0], None, own)
    early_a = mlp(rows_own, grads_own, mlp_w[0], None, own)
    early_sum, out_b, out_a = mlp_weights(
        (rows_other, grads_other, *early_b[:3]), (rows_own, grads_own, *early_a[:3]), mlp_w[0], None, own
    )
    rows_other, early_sum = lax.optimization_barrier((rows_other, early_sum))
    late_b = mlp(rows_other, grads_other, mlp_w[1], early_b[3], own)
    late_a = mlp(rows_own, grads_own, mlp_w[1], early_a[3], own)

    def plane_parts(mine, others):
        received = core_swap(others)
        return [list(pair) for pair in zip(row_parts(mine, own), row_parts(received, own))]

    grad_parts = plane_parts(late_a[3], late_b[3])
    grad_messages = row_messages(grad_parts)
    late, grad_messages = lax.optimization_barrier(((*late_b[:3], *late_a[:3]), grad_messages))
    late_sum, out_b, out_a = mlp_weights(
        (rows_other, grads_other, *late[:3]), (rows_own, grads_own, *late[3:]), mlp_w[1], (out_b, out_a), own
    )
    received, (late_sum, out_b, out_a) = lax.optimization_barrier(
        (swap_first(grad_messages), (late_sum, out_b, out_a))
    )
    grad_last = swap_first(row_turned(grad_parts, received))
    normed_two_grad = row_total(grad_parts, received, grad_last)
    out_parts = plane_parts(out_a, out_b)
    out_messages = row_messages(out_parts)
    sums = []
    for total, n in zip((early_sum, late_sum), few):
        if not aligned:
            total = total.reshape(3, n_z, n, dim).transpose(1, 0, 2, 3)
        if sums:
            total = after(total, sums[-1])
        sums.append(lax.psum_scatter(total, "z", scatter_dimension=0, tiled=False))

    normed_two_grad, out_messages = lax.optimization_barrier((normed_two_grad, out_messages))
    middle_grad, low_own, gain_two_grad = norm_two_back(middle, normed_two_grad, out_grad, gain_two)
    middle_low = jnp.concatenate([low_own, core_swap(low_own)])

    dwo = outer(middle_low, mixed, n_rows, n_z)
    dwo_parts = [[dwo[k]] for k in range(n_rows)]
    dwo_messages, middle_low = lax.optimization_barrier((row_messages(dwo_parts), middle_low))
    attended = attend_back(
        middle_low, wo, keys, keys.T, values, bias, cosine.T, sine.T, q, qt, lse, tile
    )
    out_received, dwo_received, (dq, dk, dv) = lax.optimization_barrier(
        (swap_first(out_messages), swap_first(dwo_messages), attended)
    )
    kv_to = jnp.where(first_core, dv, dk).astype(bf)
    kv_to, dq = lax.optimization_barrier((kv_to, dq))
    kv_sum = jnp.where(first_core, dk, dv) + core_swap(kv_to).astype(f32)
    kv_sum = reduce_z(kv_sum)
    dwq, dn_own, dn_other = query_back(normed, dq, wq, own)
    dwo_last, dwq = lax.optimization_barrier((swap_first(row_turned(dwo_parts, dwo_received)), dwq))
    dwo_rows = row_total(dwo_parts, dwo_received, dwo_last).astype(bf)
    dwq_parts = [[dwq[k]] for k in range(n_rows)]
    dwq_received, dwo_rows = lax.optimization_barrier((swap_first(row_messages(dwq_parts)), dwo_rows))
    dwq_last = swap_first(row_turned(dwq_parts, dwq_received))
    dwq_rows = row_total(dwq_parts, dwq_received, dwq_last).astype(bf)
    out_turned = after(row_turned(out_parts, out_received), dwq_received)
    output_rows = middle + row_total(out_parts, out_received, swap_first(out_turned))
    sum_z = lambda a: lax.psum_scatter(a.reshape(-1, block), "z", scatter_dimension=0, tiled=True)
    dwo_sum = sum_z(after(dwo_rows, sums[-1]))
    dwq_sum = sum_z(after(dwq_rows, dwo_sum)).astype(f32)
    dwo_sum = dwo_sum.astype(f32)

    kv_left, kv_right = kv_grad[:, :head], kv_grad[:, head:]
    kv_given = jnp.concatenate(
        [
            jnp.where(first_core, kv_left, kv_right),
            core_swap(jnp.where(first_core, kv_right, kv_left)),
        ]
    ).astype(f32)
    kv_low = rotate(swap_halves(kv_sum) + kv_given, kv_cosine, -kv_sine).astype(bf)
    kv_wgrad = mm(normed, kv_low, 0, 0)
    dn_kv = mm(kv_low, kv_w, 1, 1)
    input_grad, gain_one_grad = norm_one_back(
        layer_input, dn_own + dn_kv[:own], core_swap(dn_other + dn_kv[own:]), gain_one, middle_grad
    )

    mlp_sums = after(jnp.concatenate(sums, axis=1), dwq_rows).reshape(3, piece, n_rows, width)
    mlp_grads = by_row(exchange_rows([pick(mlp_sums, r ^ k, 2) for k in range(n_rows)]), axis=1)
    mlp_grads = mlp_grads.astype(f32)

    gain_rows = jnp.stack(
        [gain_one_grad.reshape(n_rows, width), gain_two_grad.reshape(n_rows, width)], axis=1
    ).reshape(n_rows, -1, head)
    small = jnp.concatenate([kv_wgrad.reshape(n_rows, width, head), gain_rows], axis=1)
    small = exchange_rows([pick(small, r ^ k) for k in range(n_rows)])
    small = functools.reduce(jnp.add, small)
    k = 1
    while k < n_z:
        small = small + axis_swap(small, "z", k)
        k *= 2
    small_other = core_swap(small)
    key_wgrad = jnp.where(first_core, small[:width], small_other[:width])
    value_wgrad = jnp.where(first_core, small_other[:width], small[:width])
    gain_sums = (small[width:] + small_other[width:]).reshape(2, width)
    return (
        output_rows.astype(bf),
        input_grad,
        shared_own,
        gain_sums[0],
        dwq_sum,
        key_wgrad,
        value_wgrad,
        dwo_sum.T,
        gain_sums[1],
        mlp_grads[0].T,
        mlp_grads[1].T,
        mlp_grads[2],
    )


def solution(mesh):
    n_rows, n_cols = mesh.shape["row"], mesh.shape["col"]
    split = Mesh(mesh.devices.reshape(n_rows, n_cols // 2, 2), ("row", "z", "core"))
    everywhere, col = ("row", "z", "core"), ("z", "core")
    in_specs = (
        P(everywhere, None),
        P(everywhere, None),
        P(everywhere, None),
        P("row", None),
        P("row", None),
        P("row"),
        P("row", col),
        P("row", None),
        P("row", None),
        P(col, "row"),
        P("row"),
        P("row", col),
        P("row", col),
        P(col, "row"),
    )
    out_specs = (
        P(everywhere, None),
        P(everywhere, None),
        P(everywhere, None),
        P("row"),
        P("row", col),
        P("row", None),
        P("row", None),
        P(col, "row"),
        P("row"),
        P("row", col),
        P("row", col),
        P(col, "row"),
    )
    return jax.shard_map(
        local, mesh=split, in_specs=in_specs, out_specs=out_specs, check_vma=False
    )
```

```python
import functools

import jax
import jax.numpy as jnp
from jax import lax
from jax.experimental import pallas as pl
from jax.experimental.pallas import tpu as pltpu
from jax.sharding import Mesh, PartitionSpec as P

norm_eps = 1e-05
rope_base = 10000.0
masked_score = -1e30
log2_e = 1.4426950408889634
f32 = jnp.float32
bf = jnp.bfloat16
vmem_bytes = 60 * 1024 * 1024


def mm(left, right, left_dim=1, right_dim=0):
    return lax.dot_general(
        left, right, (((left_dim,), (right_dim,)), ((), ())), preferred_element_type=f32
    )


def core_swap(a):
    return lax.ppermute(a, "core", [(0, 1), (1, 0)])


def axis_swap(a, axis, k):
    return lax.ppermute(a, axis, [(i, i ^ k) for i in range(lax.axis_size(axis))])


def row_swap(a, k):
    return axis_swap(a, "row", k)


def after(values, earlier):
    return lax.optimization_barrier((values, earlier))[0]


def gather_first(a):
    n = lax.axis_size("row")
    return tuple(row_swap(a, k) for k in range(1, 3 if n == 4 else n))


def gather_rest(a, first):
    if lax.axis_size("row") != 4:
        return [a, *first]
    along_x, along_y = first
    half = a.shape[0] // 2
    corner = jnp.concatenate([row_swap(along_x[:half], 2), row_swap(along_y[half:], 1)], axis=0)
    return [a, along_x, along_y, corner]


def exchange_rows(parts):
    return [parts[0]] + [row_swap(parts[k], k) for k in range(1, len(parts))]


def part_sum(parts, k, cut=slice(None)):
    return sum(term[cut].astype(f32) for term in parts[k])


def halves_of(parts):
    half = parts[0][0].shape[0] // 2
    return slice(0, half), slice(half, None)


def row_messages(parts):
    n = len(parts)
    if n != 4:
        return tuple(part_sum(parts, k).astype(bf) for k in range(1, n))
    low, high = halves_of(parts)
    return (
        jnp.stack([part_sum(parts, 1, low), part_sum(parts, 3, low)]).astype(bf),
        jnp.stack([part_sum(parts, 2, high), part_sum(parts, 3, high)]).astype(bf),
    )


def swap_first(messages):
    return tuple(row_swap(message, k) for k, message in enumerate(messages, 1))


def row_turned(parts, received):
    if len(parts) != 4:
        return ()
    low, high = halves_of(parts)
    from_x, from_y = received
    return (
        (part_sum(parts, 1, high) + from_y[1].astype(f32)).astype(bf),
        (part_sum(parts, 2, low) + from_x[1].astype(f32)).astype(bf),
    )


def row_total(parts, received, last):
    if len(parts) != 4:
        return part_sum(parts, 0) + sum(a.astype(f32) for a in received)
    from_x, from_y = received
    last_x, last_y = last
    first = jnp.concatenate([from_x[0], from_y[0]]).astype(f32)
    return part_sum(parts, 0) + first + jnp.concatenate([last_y, last_x]).astype(f32)


def by_row(pieces, axis=0):
    r = lax.axis_index("row")
    size = pieces[0].shape[axis]
    shape = list(pieces[0].shape)
    shape[axis] = size * len(pieces)
    whole = jnp.zeros(shape, pieces[0].dtype)
    for k, piece in enumerate(pieces):
        whole = lax.dynamic_update_slice_in_dim(whole, piece, (r ^ k) * size, axis)
    return whole


def reduce_z(a, cover):
    n, z = lax.axis_size("z"), lax.axis_index("z")
    size = a.shape[0] // n
    a = jnp.concatenate([lax.dynamic_slice_in_dim(a, (z ^ k) * size, size, 0) for k in range(n)])
    k = n // 2
    while k >= 1:
        half = a.shape[0] // 2
        received = axis_swap(a[half:].astype(bf), "z", k)
        if k == n // 2:
            received, cover = lax.optimization_barrier((received, cover))
        a = a[:half] + received.astype(f32)
        k //= 2
    return a, cover


def row_parts(total, rows):
    return [total[k * rows : (k + 1) * rows] for k in range(total.shape[0] // rows)]


def call(kernel, out_shape, name, flops, bytes_moved, transcendentals=0, **more):
    return pl.pallas_call(
        kernel,
        out_shape=out_shape,
        compiler_params=pltpu.CompilerParams(vmem_limit_bytes=vmem_bytes),
        cost_estimate=pl.CostEstimate(
            flops=flops, bytes_accessed=bytes_moved, transcendentals=transcendentals
        ),
        name=name,
        **more,
    )


def span_of(k, width):
    return pl.ds(pl.multiple_of((lax.axis_index("row") ^ k) * width, 128), width)


def scale_of(values):
    return lax.rsqrt(jnp.mean(values * values, axis=-1, keepdims=True) + norm_eps)


def norm_one_kernel(a_ref, b_ref, gain_ref, out_ref):
    own = a_ref.shape[0]
    for i, ref in enumerate((a_ref, b_ref)):
        values = ref[...].astype(f32)
        out_ref[i * own : (i + 1) * own, :] = (values * scale_of(values) * gain_ref[...]).astype(bf)


def norm_one(a, b, gain):
    own, dim = a.shape
    return call(
        norm_one_kernel, jax.ShapeDtypeStruct((2 * own, dim), bf), "norm_one", 8 * own * dim, 8 * own * dim
    )(a, b, gain)


def norm_two_kernel(x_ref, a_ref, b_ref, gain_ref, middle_ref, out_ref):
    middle = x_ref[...].astype(f32) + (a_ref[...] + b_ref[...])
    middle_ref[...] = middle
    out_ref[...] = (middle * scale_of(middle) * gain_ref[...]).astype(bf)


def norm_two(x, a, b, gain):
    own, dim = x.shape
    return call(
        norm_two_kernel,
        [jax.ShapeDtypeStruct((own, dim), f32), jax.ShapeDtypeStruct((own, dim), bf)],
        "norm_two",
        8 * own * dim,
        16 * own * dim,
    )(x, a, b, gain)


def through_norm(values, gain, grad):
    factor = scale_of(values)
    weighted = grad * gain
    inner = jnp.mean(weighted * values, axis=-1, keepdims=True)
    gain_part = jnp.sum(grad * values * factor, axis=0, keepdims=True)
    return factor * weighted - values * (factor * factor * factor * inner), gain_part


def norm_two_back_kernel(middle_ref, grad_ref, out_grad_ref, gain_ref, sum_ref, low_ref, gain_grad_ref):
    part, gain_grad_ref[...] = through_norm(middle_ref[...], gain_ref[...], grad_ref[...])
    total = out_grad_ref[...].astype(f32) + part
    sum_ref[...] = total
    low_ref[...] = total.astype(bf)


def norm_two_back(middle, grad, out_grad, gain):
    own, dim = middle.shape
    return call(
        norm_two_back_kernel,
        [
            jax.ShapeDtypeStruct((own, dim), f32),
            jax.ShapeDtypeStruct((own, dim), bf),
            jax.ShapeDtypeStruct((1, dim), f32),
        ],
        "norm_two_back",
        16 * own * dim,
        16 * own * dim,
    )(middle, grad, out_grad, gain)


def norm_one_back_kernel(x_ref, a_ref, b_ref, gain_ref, sum_ref, out_ref, gain_grad_ref):
    part, gain_grad_ref[...] = through_norm(
        x_ref[...].astype(f32), gain_ref[...], a_ref[...] + b_ref[...]
    )
    out_ref[...] = sum_ref[...] + part


def norm_one_back(x, a, b, gain, middle_grad):
    own, dim = x.shape
    return call(
        norm_one_back_kernel,
        [jax.ShapeDtypeStruct((own, dim), f32), jax.ShapeDtypeStruct((1, dim), f32)],
        "norm_one_back",
        16 * own * dim,
        18 * own * dim,
    )(x, a, b, gain, middle_grad)


def attend_kernel(scale, tile, rows, *refs):
    n_ref, wq_refs = refs[0], refs[1 : 1 + rows]
    k_ref, vt_ref, bias_ref, cos_ref, sin_ref = refs[1 + rows : 6 + rows]
    q_ref, qt_ref, mix_ref, lse_ref, qt_all = refs[6 + rows :]
    _, width, block = wq_refs[0].shape
    head = k_ref.shape[1]
    half = head // 2
    tiles = n_ref.shape[0] // tile
    step = pl.program_id(1)

    @pl.when(step == 0)
    def _():
        q = mm(n_ref[:, span_of(0, width)], wq_refs[0][0])
        for k in range(1, rows):
            q = q + mm(n_ref[:, span_of(k, width)], wq_refs[k][0])
        qt = q.T
        for h in range(block // head):
            first = qt[h * head : h * head + half]
            second = qt[h * head + half : (h + 1) * head]
            turned = jnp.concatenate(
                [
                    first * cos_ref[...] - second * sin_ref[...],
                    second * cos_ref[...] + first * sin_ref[...],
                ],
                axis=0,
            )
            qt_ref[h * head : (h + 1) * head, :] = turned.astype(bf)
            q_ref[:, h * head : (h + 1) * head] = turned.T.astype(bf)
            for i in range(tiles):
                qt_all[h * tiles + i] = turned[:, i * tile : (i + 1) * tile].astype(bf)

    for i in range(tiles):
        for h in range(block // head):

            @pl.when(step == h * tiles + i)
            def _(h=h, i=i):
                cols = slice(i * tile, (i + 1) * tile)
                spots = slice(h * head, (h + 1) * head)
                scores = mm(k_ref[...], qt_all[h * tiles + i]) * (scale * log2_e) + bias_ref[:, cols]
                highest = jnp.max(scores, axis=0, keepdims=True)
                weights = jnp.exp2(scores - highest)
                total = jnp.sum(weights, axis=0, keepdims=True)
                mixed = mm(vt_ref[...], weights.astype(bf)) / total
                mix_ref[cols, spots] = mixed.T.astype(bf)
                lse_ref[0, h : h + 1, cols] = highest + jnp.log2(total)


def full_spec(a):
    return pl.BlockSpec(a.shape, lambda *_: (0,) * a.ndim)


def attend(normed, wq, keys, values_t, bias, cosine_t, sine_t, tile):
    rows = len(wq)
    blocks, width, block = wq[0].shape
    tokens, dim = normed.shape
    head = keys.shape[1]
    heads = block // head
    small = (keys, values_t, bias, cosine_t, sine_t)
    return call(
        functools.partial(attend_kernel, head**-0.5, tile, rows),
        [
            jax.ShapeDtypeStruct((tokens, blocks * block), bf),
            jax.ShapeDtypeStruct((blocks * block, tokens), bf),
            jax.ShapeDtypeStruct((tokens, blocks * block), bf),
            jax.ShapeDtypeStruct((blocks, heads, tokens), f32),
        ],
        "attend",
        2 * tokens * blocks * block * (dim + 2 * keys.shape[0]),
        16 << 20,
        tokens * blocks * heads * keys.shape[0],
        grid=(blocks, heads * (tokens // tile)),
        in_specs=[full_spec(normed)]
        + [pl.BlockSpec((1, width, block), lambda z, j: (z, 0, 0))] * rows
        + [full_spec(a) for a in small],
        out_specs=[
            pl.BlockSpec((tokens, block), lambda z, j: (0, z)),
            pl.BlockSpec((block, tokens), lambda z, j: (z, 0)),
            pl.BlockSpec((tokens, block), lambda z, j: (0, z)),
            pl.BlockSpec((1, heads, tokens), lambda z, j: (z, 0, 0)),
        ],
        scratch_shapes=[pltpu.VMEM((heads * (tokens // tile), head, tile), bf)],
    )(normed, *wq, *small)


def out_kernel(own, rows, m_ref, *refs):
    wo_refs, own_ref, other_ref = refs[:rows], refs[rows], refs[rows + 1]
    _, width, block = wo_refs[0].shape
    z = pl.program_id(0)
    for k in range(rows):
        part = mm(m_ref[...], wo_refs[k][0], 1, 1)
        for ref, rest in ((own_ref, part[:own]), (other_ref, part[own:])):
            span = span_of(k, width)

            @pl.when(z == 0)
            def _():
                ref[:, span] = rest

            @pl.when(z != 0)
            def _():
                ref[:, span] += rest


def out_project(mixed, wo, own):
    rows = len(wo)
    blocks, width, block = wo[0].shape
    tokens = mixed.shape[0]
    out = jax.ShapeDtypeStruct((own, rows * width), f32)
    return call(
        functools.partial(out_kernel, own, rows),
        [out, out],
        "out_project",
        2 * tokens * blocks * block * rows * width,
        10 << 20,
        grid=(blocks,),
        in_specs=[pl.BlockSpec((tokens, block), lambda z: (0, z))]
        + [pl.BlockSpec((1, width, block), lambda z: (z, 0, 0))] * rows,
        out_specs=[pl.BlockSpec((own, rows * width), lambda z: (0, 0))] * 2,
    )(mixed, *wo)


def attend_back_kernel(scale, tile, rows, *refs):
    ml_ref, wo_refs = refs[0], refs[1 : 1 + rows]
    (k_ref, kt_ref, v_ref, bias_ref, cos_ref, sin_ref, q_ref, qt_ref, lse_ref) = refs[1 + rows : 10 + rows]
    dq_ref, dk_ref, dv_ref, do_all, dot_all = refs[10 + rows :]
    _, width, block = wo_refs[0].shape
    head = k_ref.shape[1]
    half = head // 2
    tiles = ml_ref.shape[0] // tile
    heads = block // head
    step = pl.program_id(1)

    @pl.when((pl.program_id(0) == 0) & (step == 0))
    def _():
        dk_ref[...] = jnp.zeros_like(dk_ref)
        dv_ref[...] = jnp.zeros_like(dv_ref)

    @pl.when(step == 0)
    def _():
        grad = mm(ml_ref[:, span_of(0, width)], wo_refs[0][0])
        for k in range(1, rows):
            grad = grad + mm(ml_ref[:, span_of(k, width)], wo_refs[k][0])
        do_all[...] = grad.astype(bf)
        dot_all[...] = grad.T.astype(bf)

    for i in range(tiles):
        for h in range(heads):

            @pl.when(step == h * tiles + i)
            def _(h=h, i=i):
                cols = slice(i * tile, (i + 1) * tile)
                spots = slice(h * head, (h + 1) * head)
                scores = mm(k_ref[...], qt_ref[spots, cols]) * (scale * log2_e) + bias_ref[:, cols]
                soft = jnp.exp2(scores - lse_ref[0, h : h + 1, cols])
                prob_grad = mm(v_ref[...], dot_all[spots, cols])
                row_dot = jnp.sum(soft * prob_grad, axis=0, keepdims=True)
                score_grad = (soft * (prob_grad - row_dot)).astype(bf)
                dv_ref[...] += mm(soft.astype(bf), do_all[cols, spots])
                dk_ref[...] += mm(score_grad, q_ref[cols, spots]) * scale
                dqt = mm(kt_ref[...], score_grad) * scale
                first, second = dqt[:half], dqt[half:]
                cosine, sine = cos_ref[:, cols], sin_ref[:, cols]
                turned = jnp.concatenate(
                    [first * cosine + second * sine, second * cosine - first * sine], axis=0
                )
                dq_ref[cols, spots] = turned.T.astype(bf)


def attend_back(middle_low, wo, keys, keys_t, values, bias, cosine_t, sine_t, q, qt, lse, tile):
    rows = len(wo)
    blocks, width, block = wo[0].shape
    tokens, dim = middle_low.shape
    keys_in, head = keys.shape
    heads = block // head
    small = (keys, keys_t, values, bias, cosine_t, sine_t)
    return call(
        functools.partial(attend_back_kernel, head**-0.5, tile, rows),
        [
            jax.ShapeDtypeStruct((tokens, blocks * block), bf),
            jax.ShapeDtypeStruct((keys_in, head), f32),
            jax.ShapeDtypeStruct((keys_in, head), f32),
        ],
        "attend_back",
        2 * tokens * blocks * block * (dim + 5 * keys_in),
        32 << 20,
        tokens * blocks * heads * keys_in,
        grid=(blocks, heads * (tokens // tile)),
        in_specs=[full_spec(middle_low)]
        + [pl.BlockSpec((1, width, block), lambda z, j: (z, 0, 0))] * rows
        + [full_spec(a) for a in small]
        + [
            pl.BlockSpec((tokens, block), lambda z, j: (0, z)),
            pl.BlockSpec((block, tokens), lambda z, j: (z, 0)),
            pl.BlockSpec((1, heads, tokens), lambda z, j: (z, 0, 0)),
        ],
        out_specs=[
            pl.BlockSpec((tokens, block), lambda z, j: (0, z)),
            pl.BlockSpec((keys_in, head), lambda z, j: (0, 0)),
            pl.BlockSpec((keys_in, head), lambda z, j: (0, 0)),
        ],
        scratch_shapes=[pltpu.VMEM((tokens, block), bf), pltpu.VMEM((block, tokens), bf)],
    )(middle_low, *wo, *small, q, qt, lse)


def outer_kernel(rows, width, a_ref, b_ref, out_ref):
    for k in range(rows):
        out_ref[k, 0] = mm(a_ref[:, span_of(k, width)], b_ref[...], 0, 0).astype(bf)


def outer(a, b, rows, blocks):
    tokens, dim = a.shape
    width, block = dim // rows, b.shape[1] // blocks
    return call(
        functools.partial(outer_kernel, rows, width),
        jax.ShapeDtypeStruct((rows, blocks, width, block), bf),
        "outer",
        2 * tokens * dim * b.shape[1],
        8 << 20,
        grid=(blocks,),
        in_specs=[full_spec(a), pl.BlockSpec((tokens, block), lambda z: (0, z))],
        out_specs=pl.BlockSpec((rows, 1, width, block), lambda z: (0, z, 0, 0)),
    )(a, b)


def query_back_kernel(own, rows, n_ref, dq_ref, *refs):
    wq_refs, dw_ref, own_ref, other_ref = refs[:rows], refs[rows], refs[rows + 1], refs[rows + 2]
    _, width, block = wq_refs[0].shape
    z = pl.program_id(0)
    for k in range(rows):
        span = span_of(k, width)
        dw_ref[k, 0] = mm(n_ref[:, span], dq_ref[...], 0, 0).astype(bf)
        part = mm(dq_ref[...], wq_refs[k][0], 1, 1)
        for ref, rest in ((own_ref, part[:own]), (other_ref, part[own:])):

            @pl.when(z == 0)
            def _():
                ref[:, span] = rest

            @pl.when(z != 0)
            def _():
                ref[:, span] += rest


def query_back(normed, dq, wq, own):
    rows = len(wq)
    blocks, width, block = wq[0].shape
    tokens, dim = normed.shape
    out = jax.ShapeDtypeStruct((own, dim), f32)
    return call(
        functools.partial(query_back_kernel, own, rows),
        [jax.ShapeDtypeStruct((rows, blocks, width, block), bf), out, out],
        "query_back",
        4 * tokens * dim * blocks * block,
        16 << 20,
        grid=(blocks,),
        in_specs=[full_spec(normed), pl.BlockSpec((tokens, block), lambda z: (0, z))]
        + [pl.BlockSpec((1, width, block), lambda z: (z, 0, 0))] * rows,
        out_specs=[pl.BlockSpec((rows, 1, width, block), lambda z: (0, z, 0, 0))]
        + [pl.BlockSpec((own, dim), lambda z: (0, 0))] * 2,
    )(normed, dq, *wq)


def fetch(source, target, sems, which):
    copies = []
    units = source.shape[2]
    for z in range(source.shape[0]):
        for slot, i in enumerate(which):
            copies.append(
                pltpu.make_async_copy(
                    source.at[z, i], target.at[slot, pl.ds(z * units, units)], sems.at[z, slot]
                )
            )
    for copy in copies:
        copy.start()
    for copy in copies:
        copy.wait()


def mlp_kernel(added, x_ref, g_ref, w_ref, *refs):
    prior_ref = refs[0] if added else None
    hid_ref, gg_ref, ug_ref, dx_ref, w_all, sems = refs[1:] if added else refs

    @pl.when(pl.program_id(0) == 0)
    def _():
        fetch(w_ref, w_all, sems, (0, 1, 2))

    gate = mm(x_ref[...], w_all[0], 1, 1)
    up = mm(x_ref[...], w_all[1], 1, 1)
    hidden_grad = mm(g_ref[...], w_all[2], 1, 1)
    sig = jax.nn.sigmoid(gate)
    silu = gate * sig
    hid_ref[...] = (silu * up).astype(bf)
    gate_grad = (hidden_grad * up * sig * (1.0 + gate * (1.0 - sig))).astype(bf)
    up_grad = (hidden_grad * silu).astype(bf)
    gg_ref[...] = gate_grad
    ug_ref[...] = up_grad
    dx = mm(gate_grad, w_all[0]) + mm(up_grad, w_all[1])
    if added:
        dx = dx + prior_ref[...].astype(f32)
    dx_ref[...] = dx.astype(bf)


def mlp(x, g, weights, prior, tile):
    tokens, dim = x.shape
    parts, _, few, _ = weights.shape
    units = parts * few
    rows_of = lambda width: pl.BlockSpec((tile, width), lambda t: (t, 0))
    added = prior is not None
    return call(
        functools.partial(mlp_kernel, added),
        [jax.ShapeDtypeStruct((tokens, units), bf)] * 3 + [jax.ShapeDtypeStruct((tokens, dim), bf)],
        "mlp",
        10 * tokens * units * dim,
        24 << 20,
        tokens * units,
        grid=(tokens // tile,),
        in_specs=[rows_of(dim), rows_of(dim), pl.BlockSpec(memory_space=pl.ANY)]
        + [rows_of(dim)] * added,
        out_specs=[rows_of(units), rows_of(units), rows_of(units), rows_of(dim)],
        scratch_shapes=[
            pltpu.VMEM((3, units, dim), bf),
            pltpu.SemaphoreType.DMA((parts, 3)),
        ],
    )(x, g, weights, *([prior] if added else []))


def mlp_weights_kernel(added, tiles, *refs):
    first, second, w_ref = refs[:5], refs[5:10], refs[10]
    priors = refs[11:13] if added else (None, None)
    dw_ref, out_a, out_b, total, down, sems = refs[13:] if added else refs[11:]
    step = pl.program_id(0)

    @pl.when(step == 0)
    def _():
        fetch(w_ref, down, sems, (2,))
        total[...] = jnp.zeros_like(total)

    def body(terms, prior, out):
        x_ref, g_ref, hid_ref, gg_ref, ug_ref = terms
        total[0] += mm(gg_ref[...], x_ref[...], 0, 0)
        total[1] += mm(ug_ref[...], x_ref[...], 0, 0)
        total[2] += mm(hid_ref[...], g_ref[...], 0, 0)
        part = mm(hid_ref[...], down[0])
        if prior is not None:
            part = part + prior[...].astype(f32)
        out[...] = part.astype(bf)

    @pl.when(step < tiles)
    def _():
        body(first, priors[0], out_a)

    @pl.when(step >= tiles)
    def _():
        body(second, priors[1], out_b)

    @pl.when(step == 2 * tiles - 1)
    def _():
        few = dw_ref.shape[2]
        for z in range(dw_ref.shape[0]):
            for i in range(3):
                dw_ref[z, i] = total[i, z * few : (z + 1) * few, :].astype(bf)


def mlp_weights(first, second, weights, priors, tile):
    tokens, dim = first[0].shape
    parts, _, few, _ = weights.shape
    units = parts * few
    tiles = tokens // tile
    added = priors is not None
    early = lambda width: pl.BlockSpec((tile, width), lambda t: (jnp.minimum(t, tiles - 1), 0))
    late = lambda width: pl.BlockSpec((tile, width), lambda t: (jnp.maximum(t - tiles, 0), 0))
    rows = jax.ShapeDtypeStruct((tokens, dim), bf)
    return call(
        functools.partial(mlp_weights_kernel, added, tiles),
        [jax.ShapeDtypeStruct((parts, 3, few, dim), bf), rows, rows],
        "mlp_weights",
        16 * tokens * units * dim,
        32 << 20,
        grid=(2 * tiles,),
        in_specs=[early(dim), early(dim), early(units), early(units), early(units)]
        + [late(dim), late(dim), late(units), late(units), late(units)]
        + [pl.BlockSpec(memory_space=pl.ANY)]
        + [early(dim), late(dim)] * added,
        out_specs=[
            pl.BlockSpec((parts, 3, few, dim), lambda t: (0, 0, 0, 0)),
            early(dim),
            late(dim),
        ],
        scratch_shapes=[
            pltpu.VMEM((3, units, dim), f32),
            pltpu.VMEM((1, units, dim), bf),
            pltpu.SemaphoreType.DMA((parts, 1)),
        ],
    )(*first, *second, weights, *(priors if added else []))


def rotate(values, cosine, sine):
    half = values.shape[1] // 2
    first, second = values[:, :half], values[:, half:]
    return jnp.concatenate([first * cosine - second * sine, second * cosine + first * sine], axis=1)


def local(layer_input, out_grad, kv_grad, lengths, token_deal, attn_gain, query_weight, key_weight,
          value_weight, out_weight, mlp_gain, gate_weight, up_weight, down_weight):
    r, z, c = lax.axis_index("row"), lax.axis_index("z"), lax.axis_index("core")
    n_rows, n_z = lax.axis_size("row"), lax.axis_size("z")
    own, dim = layer_input.shape
    width, block = query_weight.shape
    head = key_weight.shape[1]
    units = gate_weight.shape[1]
    piece = units // n_rows
    pick = lambda a, i, axis=0: lax.dynamic_index_in_dim(a, i, axis, keepdims=False)
    first_core = c == 0

    wq_z = lax.all_gather(query_weight.astype(bf), "z", axis=0)
    mlp_own = jnp.stack(
        [gate_weight.astype(bf).T, up_weight.astype(bf).T, down_weight.astype(bf)]
    ).reshape(3, n_rows, piece, width)
    mlp_parts = exchange_rows([pick(mlp_own, r ^ k, 1) for k in range(n_rows)])
    gains = jnp.concatenate([attn_gain, mlp_gain]).astype(bf).reshape(-1, head)
    small = jnp.concatenate([jnp.where(first_core, key_weight, value_weight).astype(bf), gains])
    small = by_row(exchange_rows([small] * n_rows)).reshape(n_rows, -1, head)
    kv_w = small[:, :width].reshape(dim, head)
    gains = small[:, width:].reshape(n_rows, 2, width).astype(f32)
    gain_one, gain_two = gains[:, 0].reshape(1, dim), gains[:, 1].reshape(1, dim)

    chip = 2 * own
    deal = token_deal[0]
    ends = jnp.cumsum(lengths[0])

    def start_of(initial):
        return jnp.sum(jnp.where(ends[None, :] <= initial[:, None], lengths[0][None, :], 0), axis=1)

    swap_halves = lambda a: jnp.where(first_core, a, jnp.roll(a, own, axis=0))
    initial = swap_halves(lax.dynamic_slice_in_dim(deal, z * chip, chip, 0))
    start = start_of(initial)
    angles = (initial - start).astype(f32)[:, None] * (
        rope_base ** (-jnp.arange(head // 2, dtype=f32) / (head // 2))
    )
    cosine, sine = jnp.cos(angles), jnp.sin(angles)
    bias = jnp.where(
        (deal[:, None] >= start[None, :]) & (deal[:, None] <= initial[None, :]),
        0.0,
        masked_score,
    ).astype(f32)
    kv_cosine, kv_sine = jnp.where(first_core, cosine, 1.0), jnp.where(first_core, sine, 0.0)

    normed = norm_one(layer_input, core_swap(layer_input), gain_one)
    kv_own = swap_halves(rotate(mm(normed, kv_w), kv_cosine, kv_sine).astype(bf))
    mlp_parts = after(mlp_parts, kv_own)
    wo_low = after(out_weight.astype(bf).T, wq_z)
    wo_z = lax.all_gather(wo_low, "z", axis=0)
    kv_mine = lax.all_gather(after(kv_own, wo_low), "z", axis=0, tiled=True)
    wq_z = after(wq_z, mlp_parts)
    wq_first, kv_mine = lax.optimization_barrier((gather_first(wq_z), kv_mine))
    kv_other = core_swap(kv_mine)
    keys = jnp.where(first_core, kv_mine, kv_other)
    values = jnp.where(first_core, kv_other, kv_mine)
    mine = lambda a: lax.dynamic_slice_in_dim(a, z * chip + c * own, own, 0)
    shared_own = jnp.concatenate([mine(keys), mine(values)], axis=1)

    mlp_parts = by_row(mlp_parts, axis=2)
    late_units = piece * 4 // 11
    cuts = [slice(0, piece - late_units), slice(piece - late_units, piece)]
    few = [cut.stop - cut.start for cut in cuts]
    mlp_w = []
    for cut in cuts:
        earlier = mlp_w[-1] if mlp_w else wo_z
        mlp_w.append(lax.all_gather(after(mlp_parts[:, cut], earlier), "z", axis=0))
    aligned = all(n % 16 == 0 for n in few)
    if not aligned:
        mlp_w = [
            w.transpose(1, 0, 2, 3).reshape(1, 3, n_z * n, dim) for w, n in zip(mlp_w, few)
        ]

    wq = gather_rest(wq_z, wq_first)
    wo_z, grads = after((wo_z, out_grad), wq)
    tile = own
    attended = attend(normed, wq, keys, values.T, bias, cosine.T, sine.T, tile)
    wo_first, grads_first, (q, qt, mixed, lse) = lax.optimization_barrier(
        (gather_first(wo_z), gather_first(grads), attended)
    )
    wo = gather_rest(wo_z, wo_first)
    att_own, att_other = out_project(mixed, wo, own)
    middle, normed_two = norm_two(layer_input, att_own, core_swap(att_other), gain_two)

    grads_own = jnp.concatenate(gather_rest(grads, after(grads_first, wo)))
    grads_other = core_swap(grads_own)
    rows_own = jnp.concatenate(gather_rest(normed_two, gather_first(normed_two)))
    rows_other = core_swap(rows_own)
    early_b = mlp(rows_other, grads_other, mlp_w[0], None, own)
    early_a = mlp(rows_own, grads_own, mlp_w[0], None, own)
    early_sum, out_b, out_a = mlp_weights(
        (rows_other, grads_other, *early_b[:3]), (rows_own, grads_own, *early_a[:3]), mlp_w[0], None, own
    )
    rows_other, early_sum = lax.optimization_barrier((rows_other, early_sum))
    late_b = mlp(rows_other, grads_other, mlp_w[1], early_b[3], own)
    late_a = mlp(rows_own, grads_own, mlp_w[1], early_a[3], own)

    def plane_parts(mine, others):
        received = core_swap(others)
        return [list(pair) for pair in zip(row_parts(mine, own), row_parts(received, own))]

    grad_parts = plane_parts(late_a[3], late_b[3])
    grad_messages = row_messages(grad_parts)
    late, grad_messages = lax.optimization_barrier(((*late_b[:3], *late_a[:3]), grad_messages))
    late_sum, out_b, out_a = mlp_weights(
        (rows_other, grads_other, *late[:3]), (rows_own, grads_own, *late[3:]), mlp_w[1], (out_b, out_a), own
    )
    received, (late_sum, out_b, out_a) = lax.optimization_barrier(
        (swap_first(grad_messages), (late_sum, out_b, out_a))
    )
    grad_last = swap_first(row_turned(grad_parts, received))
    normed_two_grad = row_total(grad_parts, received, grad_last)
    out_parts = plane_parts(out_a, out_b)
    out_messages = row_messages(out_parts)

    def sum_mlp(total):
        if not aligned:
            total = total.reshape(3, n_z, -1, dim).transpose(1, 0, 2, 3)
        return lax.psum_scatter(total, "z", scatter_dimension=0, tiled=False)

    early_sum = sum_mlp(early_sum)
    late_sum = sum_mlp(after(late_sum, early_sum))

    normed_two_grad, out_messages = lax.optimization_barrier((normed_two_grad, out_messages))
    middle_grad, low_own, gain_two_grad = norm_two_back(middle, normed_two_grad, out_grad, gain_two)
    middle_low = jnp.concatenate([low_own, core_swap(low_own)])

    dwo = outer(middle_low, mixed, n_rows, n_z)
    dwo_parts = [[dwo[k]] for k in range(n_rows)]
    dwo_messages, middle_low = lax.optimization_barrier((row_messages(dwo_parts), middle_low))
    attended = attend_back(
        middle_low, wo, keys, keys.T, values, bias, cosine.T, sine.T, q, qt, lse, tile
    )
    out_received, dwo_received, (dq, dk, dv) = lax.optimization_barrier(
        (swap_first(out_messages), swap_first(dwo_messages), attended)
    )
    kv_to = jnp.where(first_core, dv, dk).astype(bf)
    kv_to, dq = lax.optimization_barrier((kv_to, dq))
    kv_sum = jnp.where(first_core, dk, dv) + core_swap(kv_to).astype(f32)
    dwq, *dn = query_back(normed, dq, wq, own)
    kv_sum, (dn_own, dn_other) = reduce_z(kv_sum, dn)
    dwo_last, dwq = lax.optimization_barrier((swap_first(row_turned(dwo_parts, dwo_received)), dwq))
    dwo_rows = row_total(dwo_parts, dwo_received, dwo_last).astype(bf)
    dwq_parts = [[dwq[k]] for k in range(n_rows)]
    dwq_received = swap_first(row_messages(dwq_parts))
    dwq_turned = row_turned(dwq_parts, dwq_received)
    dwq_last = swap_first(dwq_turned)
    dwq_rows = row_total(dwq_parts, dwq_received, dwq_last).astype(bf)
    out_turned = after(row_turned(out_parts, out_received), dwq_turned)
    output_rows = middle + row_total(out_parts, out_received, swap_first(out_turned))
    sum_z = lambda a: lax.psum_scatter(a.reshape(-1, block), "z", scatter_dimension=0, tiled=True)
    dwo_sum = sum_z(after(dwo_rows, late_sum))
    dwq_sum = sum_z(after(dwq_rows, dwo_sum)).astype(f32)
    dwo_sum = dwo_sum.astype(f32)

    kv_left, kv_right = kv_grad[:, :head], kv_grad[:, head:]
    kv_given = jnp.concatenate(
        [
            jnp.where(first_core, kv_left, kv_right),
            core_swap(jnp.where(first_core, kv_right, kv_left)),
        ]
    ).astype(f32)
    kv_low = rotate(swap_halves(kv_sum) + kv_given, kv_cosine, -kv_sine).astype(bf)
    kv_wgrad = mm(normed, kv_low, 0, 0)
    dn_kv = mm(kv_low, kv_w, 1, 1)
    input_grad, gain_one_grad = norm_one_back(
        layer_input, dn_own + dn_kv[:own], core_swap(dn_other + dn_kv[own:]), gain_one, middle_grad
    )

    sums = [a.reshape(3, -1, dim) for a in after((early_sum, late_sum), dwq_turned)]
    to_row = lambda k: jnp.concatenate(
        [lax.dynamic_slice_in_dim(a, (r ^ k) * width, width, 2) for a in sums], axis=1
    )
    mlp_grads = by_row(exchange_rows([to_row(k) for k in range(n_rows)]), axis=1)
    mlp_grads = mlp_grads.astype(f32)

    gain_rows = jnp.stack(
        [gain_one_grad.reshape(n_rows, width), gain_two_grad.reshape(n_rows, width)], axis=1
    ).reshape(n_rows, -1, head)
    small = jnp.concatenate([kv_wgrad.reshape(n_rows, width, head), gain_rows], axis=1)
    small = exchange_rows([pick(small, r ^ k) for k in range(n_rows)])
    small = functools.reduce(jnp.add, small)
    k = 1
    while k < n_z:
        small = small + axis_swap(small, "z", k)
        k *= 2
    small_other = core_swap(small)
    key_wgrad = jnp.where(first_core, small[:width], small_other[:width])
    value_wgrad = jnp.where(first_core, small_other[:width], small[:width])
    gain_sums = (small[width:] + small_other[width:]).reshape(2, width)
    return (
        output_rows.astype(bf),
        input_grad,
        shared_own,
        gain_sums[0],
        dwq_sum,
        key_wgrad,
        value_wgrad,
        dwo_sum.T,
        gain_sums[1],
        mlp_grads[0].T,
        mlp_grads[1].T,
        mlp_grads[2],
    )


def solution(mesh):
    n_rows, n_cols = mesh.shape["row"], mesh.shape["col"]
    split = Mesh(mesh.devices.reshape(n_rows, n_cols // 2, 2), ("row", "z", "core"))
    everywhere, col = ("row", "z", "core"), ("z", "core")
    in_specs = (
        P(everywhere, None),
        P(everywhere, None),
        P(everywhere, None),
        P("row", None),
        P("row", None),
        P("row"),
        P("row", col),
        P("row", None),
        P("row", None),
        P(col, "row"),
        P("row"),
        P("row", col),
        P("row", col),
        P(col, "row"),
    )
    out_specs = (
        P(everywhere, None),
        P(everywhere, None),
        P(everywhere, None),
        P("row"),
        P("row", col),
        P("row", None),
        P("row", None),
        P(col, "row"),
        P("row"),
        P("row", col),
        P("row", col),
        P(col, "row"),
    )
    return jax.shard_map(
        local, mesh=split, in_specs=in_specs, out_specs=out_specs, check_vma=False
    )
```
